1024 devices in a mesh: dp: 32 (over z_lo, x, core), expert: 32 (over y, z_hi).
Axes of the slice: x: 4, y: 8, z: 16 (z_hi: 4, z_lo: 4; z = z_hi * 4 + z_lo), core: 2. Of those that a mesh axis runs over, the one named last changes fastest.
Arguments:
- tokens: bfloat16 [8192, 2048], P('dp', 'expert'), may hold values from -6 to 6
- out_grad: bfloat16 [8192, 2048], P('dp', 'expert'), may hold values from -6 to 6
- expert_out: bfloat16 [8192, 2048], P('dp', 'expert'), may hold values from -0.119628906 to 0.119628906
- router_probs: float32 [8192, 32], P('dp'), may hold values from 0 to 1, as said below
- expert_index: int32 [8192, 1], P('dp'), may hold values from 0 to 31; in each aligned block of 256 rows (0 to 255, 256 to 511, ...) at most 10 rows name the same one
- in_weight: bfloat16 [32, 2, 5120, 2048], P('expert', None, 'dp'), may hold values from -0.125 to 0.125
- down_weight: bfloat16 [32, 5120, 2048], P('expert', 'dp'), may hold values from -0.078125 to 0.078125
- router_weight: bfloat16 [2048, 32], P('expert'), may hold values from -6 to 6
Outputs:
- token_grad: bfloat16 [8192, 2048], P('dp', 'expert')
- in_weight_grad: bfloat16 [32, 2, 5120, 2048], P('expert', None, 'dp')
- router_grad: float32 [2048, 32], P('expert')
The draws below stay inside these ranges and needn't reach their ends.
Inputs may be any that keep to these rules, and one draw needn't show every extreme that they name: `expert_index`: in each aligned block of 256 tokens (one group) no expert is chosen more than 10 times, so no token is dropped. `router_probs`: each row is positive and sums to one.
All inputs are finite; a program needn't handle non-finite values.
Results may differ from the reference program's by a relative error of at most 0.0057.
Values may be sent and summed in bfloat16 or wider, within the bound.
No kernel may reach another device: no remote copies, remote signals or barrier semaphores. Data moves between devices by JAX's collectives and lax.ppermute only.
A program may use at most 64 MiB of HBM per device.

```python
import math
from functools import partial
import jax
import jax.numpy as jnp
import numpy as np
from jax import lax

D = 2048
FF = 5120
TOK_ROW = 256
E = 32
TOKENS = 8192
CAP = 10
N_DP = 32


def draw_router_probs(key, part):
    logits = 1.5 * jax.random.normal(key, (TOKENS, E), jnp.float32)
    return jax.nn.softmax(logits, axis=1)


def levels(rng, dims, cuts, least, largest):
    factor_of, own = 1.0, jax.random.fold_in(rng, 6)
    for dim, blocks in cuts:
        draws = jnp.exp(jax.random.uniform(jax.random.fold_in(own, dim), (blocks,), jnp.float32, least / len(cuts), largest / len(cuts)))
        factor_of = factor_of * jnp.repeat(draws, dims[dim] // blocks).reshape([-1 if axis == dim else 1 for axis in range(len(dims))])
    return factor_of


def shared_out(stream_key, own, number, rows, count, top, most, skew):
    order = jax.random.permutation(stream_key, count)
    crowded, ordinary = shares(count, rows * top, most, skew, True), shares(count, rows * top, most, skew, False)
    places = jnp.arange(count)

    def named(tallies, rotation):
        used = int((tallies > 0).sum())
        fixed = max(1, used // 4)
        passed = fixed + (places - fixed + rotation * (used - fixed)) % max(1, count - fixed)
        return jnp.zeros((count,), jnp.int32).at[order[jnp.where(places < fixed, places, passed)]].set(jnp.asarray(tallies, jnp.int32))

    tallies = jnp.where(number % 4 == 0, named(crowded, number // 4), named(ordinary, number - number // 4 - 1))
    mixed = jax.random.permutation(jax.random.fold_in(own, 3), count)
    source_of, receiver = mixed[0:count // 2 * 2:2], mixed[1:count // 2 * 2:2]
    slack = jnp.minimum(tallies[source_of] - 1, most - tallies[receiver]) // 2
    slack = jnp.where((source_of == order[0]) | (receiver == order[0]) | (tallies[receiver] == 0), 0, jnp.maximum(slack, 0))
    passed = jax.random.randint(jax.random.fold_in(own, 4), (count // 2,), 0, 1 << 20) % (slack + 1)
    tallies = tallies.at[source_of].add(-passed).at[receiver].add(passed)
    labels = jnp.searchsorted(jnp.cumsum(tallies), jnp.arange(rows * top), side="right").astype(jnp.int32)
    table = labels.reshape(top, rows).T
    table = table[jax.random.permutation(jax.random.fold_in(own, 1), rows)]
    rotation = jax.random.randint(jax.random.fold_in(own, 2), (rows, 1), 0, top)
    return jnp.take_along_axis(table, (jnp.arange(top)[None, :] + rotation) % top, axis=1)


def shares(amount, total, bound, skew, full):
    portions = [(1 << 20) // math.isqrt(grade ** skew) + 1 for grade in range(1, amount + 1)]
    largest = bound if full else min(bound, max(-(-total // amount), total * portions[0] // sum(portions)))
    least = 1 if total - largest >= amount - 1 else 0
    given, rest = [largest] + [least] * (amount - 1), total - largest - least * (amount - 1)
    while rest > 0:
        movable = [i for i in range(1, amount) if given[i] < largest] or [i for i in range(1, amount) if given[i] < bound]
        pool, remaining = sum([portions[i] for i in movable]), rest
        for i in movable:
            more = min(bound - given[i], max(1, remaining * portions[i] // pool), rest)
            given[i] = given[i] + more
            rest = rest - more
    return np.array(given)


def gaussian(stream_key, shape, scale, most, cuts=(), kind=jnp.bfloat16):
    loudness = levels(stream_key, shape, cuts, -0.22, 0.18) if cuts else 1.0
    values = jax.random.normal(stream_key, shape, jnp.float32) * scale * loudness
    return jnp.minimum(jnp.maximum(values, -most), most).astype(kind)


def setup_inputs(seed: int = 0) -> dict:
    key_of = jax.random.split(jax.random.key(seed), 9)
    tokens = gaussian(key_of[0], (TOKENS, D), 1.0, 6.0, ((0, 32), (1, 32)))
    out_grad = gaussian(key_of[1], (TOKENS, D), 1.0, 6.0, ((0, 32), (1, 32)))
    expert_out = gaussian(key_of[2], (TOKENS, D), 0.02, 0.119628906, ((0, 32), (1, 32)))
    router_probs = draw_router_probs(jax.random.fold_in(key_of[8], 71), 0)
    expert_index_keys = jax.random.split(jax.random.fold_in(key_of[4], 1), TOKENS // TOK_ROW)
    expert_index_turns = jax.random.permutation(jax.random.fold_in(key_of[4], 3), TOKENS // TOK_ROW)
    expert_index = jax.vmap(lambda own, number: shared_out(jax.random.fold_in(key_of[4], 2), own, number, TOK_ROW, E, 1, CAP, 2))(expert_index_keys, expert_index_turns).reshape((TOKENS, 1))
    in_weight = gaussian(key_of[5], (E, 2, FF, D), D ** -0.5, 0.125, ((0, 32), (2, 32)))
    down_weight = gaussian(key_of[6], (E, FF, D), FF ** -0.5, 0.078125, ((0, 32), (1, 32)))
    router_weight = gaussian(key_of[7], (D, E), 1.0, 6.0, ((0, 32),))
    return {"tokens": tokens, "out_grad": out_grad, "expert_out": expert_out, "router_probs": router_probs, "expert_index": expert_index, "in_weight": in_weight, "down_weight": down_weight, "router_weight": router_weight}


aux_coef = 0.2

def slot_numbers(routes):
    width = routes.shape[1]
    same_expert = routes[:, :, None] == routes[:, None, :]
    position = jnp.arange(width, dtype=jnp.int32)
    before = position[None, :] < position[:, None]
    return lax.optimization_barrier(jnp.sum((same_expert & before[None]).astype(jnp.int32), axis=2))

def one_hot(routes, slot_ids, experts, capacity):
    expert_hit = routes[..., None] == jnp.arange(experts, dtype=jnp.int32)
    slot_hit = slot_ids[..., None] == jnp.arange(capacity, dtype=jnp.int32)
    return (expert_hit[..., :, None] & slot_hit[..., None, :]).astype(jnp.float32)

def gelu_parts(pre_act, upstream):
    gelu_value, pullback = jax.vjp(partial(jax.nn.gelu, approximate=True), pre_act)
    return (gelu_value, pullback(upstream)[0])

def expert_backward(pieces):
    row_tokens, row_grads, weights, down = pieces
    contract_last = (((1,), (1,)), ((), ()))
    contract_first = (((0,), (0,)), ((), ()))
    gate_pre = lax.dot_general(row_tokens, weights[0], contract_last, preferred_element_type=jnp.float32)
    up_pre = lax.dot_general(row_tokens, weights[1], contract_last, preferred_element_type=jnp.float32)
    hidden_grad = lax.dot_general(row_grads, down, contract_last, preferred_element_type=jnp.float32)
    gate_act, gate_back = gelu_parts(gate_pre, hidden_grad * up_pre)
    gate_grad = gate_back.astype(jnp.bfloat16)
    up_grad = (hidden_grad * gate_act).astype(jnp.bfloat16)
    w_gate_grad = lax.dot_general(gate_grad, row_tokens, contract_first, preferred_element_type=jnp.float32)
    w_up_grad = lax.dot_general(up_grad, row_tokens, contract_first, preferred_element_type=jnp.float32)
    partial_in = jnp.dot(gate_grad, weights[0], preferred_element_type=jnp.float32)
    partial_in = partial_in + jnp.dot(up_grad, weights[1], preferred_element_type=jnp.float32)
    return (jnp.stack([w_gate_grad, w_up_grad]).astype(jnp.bfloat16), partial_in)

def reference(tokens, out_grad, expert_out, router_probs, expert_index, in_weight, down_weight, router_weight):
    groups = N_DP
    experts = router_probs.shape[1]
    capacity = CAP
    feature_width = tokens.shape[1]
    routes = expert_index[:, 0].reshape(groups, TOK_ROW)
    slot_ids = slot_numbers(routes)
    dispatch_mask = one_hot(routes, slot_ids, experts, capacity)
    chosen = lax.optimization_barrier(jnp.sum(dispatch_mask, axis=3)).reshape(TOKENS, experts)
    gate = lax.optimization_barrier(jnp.sum(router_probs * chosen, axis=1))
    gated_dy = (gate[:, None] * out_grad.astype(jnp.float32)).astype(jnp.bfloat16)

    def dispatch(values):
        grouped = values.astype(jnp.float32).reshape(groups, TOK_ROW, feature_width)
        placed = jnp.einsum('gtec,gtf->egcf', dispatch_mask, grouped, precision=lax.Precision.HIGHEST)
        return placed.astype(jnp.bfloat16).reshape(experts, groups * capacity, feature_width)
    row_tokens = dispatch(tokens)
    row_grads = dispatch(gated_dy)
    weight_grads, partials = lax.map(expert_backward, (row_tokens, row_grads, in_weight, down_weight))
    partials = partials.reshape(experts, groups, capacity, feature_width)
    combined = jnp.einsum('gtec,egcf->gtf', dispatch_mask, partials, precision=lax.Precision.HIGHEST)
    combined = combined.reshape(TOKENS, feature_width)
    gate_dot = lax.optimization_barrier(jnp.sum(out_grad.astype(jnp.float32) * expert_out.astype(jnp.float32), axis=1))
    counts = lax.optimization_barrier(jnp.sum(chosen, axis=0))
    prob_grad = chosen * gate_dot[:, None] + aux_coef * experts * counts[None, :] / TOKENS
    logit_grad = router_probs * (prob_grad - lax.optimization_barrier(jnp.sum(router_probs * prob_grad, axis=1, keepdims=True)))
    logit_grad = logit_grad.astype(jnp.bfloat16)
    router_grad = lax.dot_general(tokens, logit_grad, (((0,), (0,)), ((), ())), preferred_element_type=jnp.float32)
    router_term = lax.dot_general(logit_grad, router_weight, (((1,), (1,)), ((), ())), preferred_element_type=jnp.float32)
    token_grad = (combined + router_term).astype(jnp.bfloat16)
    return (token_grad, weight_grads, router_grad)
```

```python
import jax
import jax.numpy as jnp
from jax import lax
from jax.experimental import pallas as pl
from jax.experimental.pallas import tpu as pltpu
from jax.sharding import Mesh, PartitionSpec as P

ZL, X, CORE, Y, ZH = 4, 4, 2, 8, 4
EX = ("y", "zh")
DP = ("zl", "x", "core")
E = 32
CAP = 10
T = 256
F = 64
D = 2048
KT = 2 * D // 128
AUX = 0.2
F32, BF16 = jnp.float32, jnp.bfloat16
CONTRACT_LAST = (((1,), (1,)), ((), ()))
CONTRACT_FIRST = (((0,), (0,)), ((), ()))


def vmem(n):
    return [pl.BlockSpec(memory_space=pltpu.VMEM)] * n


def iota(shape, dim):
    return lax.broadcasted_iota(jnp.int32, shape, dim)


def slots(idx):
    hit = iota((E, T), 0) == idx
    hot = jnp.where(hit, 1.0, 0.0).astype(F32)
    earlier = jnp.where(iota((T, T), 0) < iota((T, T), 1), 1.0, 0.0).astype(BF16)
    before = jnp.dot(hot.astype(BF16), earlier, preferred_element_type=F32)
    return hot, jnp.sum(hot * before, axis=0, keepdims=True)


def dispatch_kernel(tok, og, eo, probs, idx_ref, out):
    idx = idx_ref[...]
    hot, slot = slots(idx)
    gate = jnp.sum(probs[...] * hot, axis=0, keepdims=True)
    grad = og[...].astype(F32)
    gated = (gate * grad).astype(BF16)
    dot = jnp.sum(grad * eo[...].astype(F32), axis=0, keepdims=True)
    row = iota((E * 16, T), 0)
    sel = jnp.where(
        (lax.shift_right_logical(row, 4) == idx) & (lax.bitwise_and(row, 15) == slot.astype(jnp.int32)),
        1.0,
        0.0,
    ).astype(BF16)
    both = jnp.concatenate([tok[...], gated], axis=0)
    sent = lax.dot_general(sel, both, CONTRACT_LAST, preferred_element_type=F32)
    h0 = dot.astype(BF16).astype(F32)
    h1 = (dot - h0).astype(BF16).astype(F32)
    h2 = dot - h0 - h1
    line = iota((16, 128), 0)
    extra = jnp.zeros((16, 128), F32)
    for i, h in enumerate((h0, h1, h2)):
        for j in range(2):
            extra = extra + jnp.where(line == CAP + 2 * i + j, h[:, 128 * j : 128 * (j + 1)], 0.0)
    out[...] = (sent.reshape(E, 16, 128) + extra[None]).astype(BF16)


def pack_kernel(got, idx_ref, out, dot_ref):
    lane = iota((16, 128), 1)
    low = lane < F
    tail = [jnp.zeros((8, 128), F32) for _ in range(KT // 4)]
    line = iota((8, 128), 0)
    total = jnp.zeros((16, 128), F32)
    for j in range(E // 2):
        a = got[2 * j].astype(F32)
        b = got[2 * j + 1].astype(F32)
        total = total + a + b
        t = jnp.where(low, a, pltpu.roll(b, F, 1))
        g = jnp.where(low, pltpu.roll(a, F, 1), b)
        for k, v in ((j, t), (j + E // 2, g)):
            head = v[:8].astype(BF16)
            for z in range(ZL):
                out[z, k] = head
            i = k % 4
            rest = v[8:] if i == 0 else pltpu.roll(v[8:], 2 * i, 0)
            tail[k // 4] = jnp.where((line >= 2 * i) & (line < 2 * i + 2), rest, tail[k // 4])
    for m in range(KT // 4):
        for z in range(ZL):
            out[z, KT + m] = tail[m].astype(BF16)
    hot = jnp.where(iota((128, T), 0) == idx_ref[...], 1.0, 0.0).astype(BF16)
    counts = lax.dot_general(jnp.ones((8, T), BF16), hot, CONTRACT_LAST, preferred_element_type=F32)
    for z in range(ZL):
        out[z, KT + KT // 4] = counts.astype(BF16)
    pick = jnp.where((line >= 2) & (lax.bitwise_and(line, 1) == 0), 1.0, 0.0)
    pick1 = jnp.where((line >= 2) & (lax.bitwise_and(line, 1) == 1), 1.0, 0.0)
    dot_ref[:, :128] = jnp.sum(total[8:] * pick, axis=0, keepdims=True)
    dot_ref[:, 128:] = jnp.sum(total[8:] * pick1, axis=0, keepdims=True)


def combine_kernel(ret, idx_ref, lg, rw, out):
    idx = idx_ref[...]
    _, slot = slots(idx)
    slot = slot.astype(jnp.int32)
    row = iota((E * 8, T), 0)
    mine = lax.shift_right_logical(row, 3) == idx
    c = lax.bitwise_and(row, 7)
    r = ret[...].reshape(E * 8, 128)
    acc = lax.dot_general(rw[...], lg[...], CONTRACT_FIRST, preferred_element_type=F32)
    for h in range(2):
        sel = jnp.where(mine & (c < 5) & (c + 5 * h == slot), 1.0, 0.0).astype(BF16)
        p = lax.dot_general(r, sel, CONTRACT_FIRST, preferred_element_type=F32)
        acc = acc + p[F * h : F * (h + 1)]
    out[...] = acc.astype(BF16)


def rows_of(got):
    n = got.shape[0]
    head = got[:, :KT].transpose(0, 2, 1, 3).reshape(n * 8, 2 * D)
    tail = got[:, KT : KT + KT // 4].reshape(n, KT // 4, 4, 2, 128)
    tail = tail.transpose(0, 3, 1, 2, 4).reshape(n * 2, 2 * D)
    return jnp.concatenate([head, tail], axis=0)


def backward(rows, in_w, down_w):
    tok, dy = rows[:, :D], rows[:, D:]
    gate_pre = lax.dot_general(tok, in_w[0], CONTRACT_LAST, preferred_element_type=F32)
    up_pre = lax.dot_general(tok, in_w[1], CONTRACT_LAST, preferred_element_type=F32)
    hidden = lax.dot_general(dy, down_w, CONTRACT_LAST, preferred_element_type=F32)
    act, pull = jax.vjp(lambda v: jax.nn.gelu(v, approximate=True), gate_pre)
    gate_grad = pull(hidden * up_pre)[0].astype(BF16)
    up_grad = (hidden * act).astype(BF16)
    return gate_grad, up_grad


def per_device(tokens, out_grad, expert_out, probs, idx, in_weight, down_weight, router_weight):
    tok, og, eo, pt, ix = tokens.T, out_grad.T, expert_out.T, probs.T, idx.T
    in_w, down_w = in_weight[0], down_weight[0]
    send = pl.pallas_call(
        dispatch_kernel,
        out_shape=jax.ShapeDtypeStruct((E, 16, 128), BF16),
        in_specs=vmem(5),
        out_specs=vmem(1)[0],
        name="dispatch",
    )(tok, og, eo, pt, ix)
    got = lax.all_to_all(send, EX, 0, 0, tiled=True)
    packed, gate_dot = pl.pallas_call(
        pack_kernel,
        out_shape=(
            jax.ShapeDtypeStruct((ZL, KT + KT // 4 + 1, 8, 128), BF16),
            jax.ShapeDtypeStruct((1, T), F32),
        ),
        in_specs=vmem(2),
        out_specs=tuple(vmem(2)),
        name="pack",
    )(got, ix)
    line = lax.all_to_all(packed, "zl", 0, 0, tiled=True)
    plane = lax.all_to_all(jnp.broadcast_to(line, (X, *line.shape)), "x", 0, 0, tiled=True)
    own = plane.reshape(X * ZL, *line.shape[1:])
    other = lax.ppermute(own, "core", [(0, 1), (1, 0)])

    counts = jnp.sum(own[:, -1, 0, :E].astype(F32), axis=0) + jnp.sum(
        other[:, -1, 0, :E].astype(F32), axis=0
    )
    hot = (jnp.arange(E, dtype=jnp.int32)[:, None] == ix).astype(F32)
    prob_grad = hot * gate_dot + (AUX * E * counts / (T * E))[:, None]
    lg = (pt * (prob_grad - jnp.sum(pt * prob_grad, axis=0, keepdims=True))).astype(BF16)
    router_part = lax.dot_general(lg, tok, CONTRACT_LAST, preferred_element_type=F32)
    copies = jnp.broadcast_to(router_part.reshape(1, 1, E * F), (E, 1, E * F))
    router_sum = jnp.sum(lax.all_to_all(copies, DP, 0, 0, tiled=True), axis=(0, 1)).reshape(E, F)

    own_rows, other_rows = rows_of(own), rows_of(other)
    gg_o, ug_o = backward(other_rows, in_w, down_w)
    gg_m, ug_m = backward(own_rows, in_w, down_w)

    def row_grad(gg, ug):
        return jnp.dot(gg, in_w[0], preferred_element_type=F32) + jnp.dot(
            ug, in_w[1], preferred_element_type=F32
        )

    from_core = lax.ppermute(row_grad(gg_o, ug_o).astype(BF16), "core", [(0, 1), (1, 0)])
    mine = row_grad(gg_m, ug_m) + from_core.astype(F32)
    half = mine.astype(BF16)
    n = X * ZL
    to_x = jnp.concatenate(
        [half[: 8 * n].reshape(X, 8 * ZL, D), half[8 * n :].reshape(X, 2 * ZL, D)], axis=1
    )
    part = jnp.sum(lax.all_to_all(to_x, "x", 0, 0, tiled=True).astype(F32), axis=0).astype(BF16)
    to_z = jnp.concatenate(
        [part[: 8 * ZL].reshape(ZL, 8, D), part[8 * ZL :].reshape(ZL, 2, D)], axis=1
    )
    done = jnp.sum(lax.all_to_all(to_z, "zl", 0, 0, tiled=True).astype(F32), axis=0).astype(BF16)
    back = done.reshape(2, 5, E, F).transpose(2, 1, 0, 3).reshape(E, 5, 128)
    back = jnp.pad(back, ((0, 0), (0, 3), (0, 0)))
    ret = lax.all_to_all(back, EX, 0, 0, tiled=True)

    def weight_grad(a, b):
        return lax.dot_general(a, own_rows[:, :D], CONTRACT_FIRST, preferred_element_type=F32) + (
            lax.dot_general(b, other_rows[:, :D], CONTRACT_FIRST, preferred_element_type=F32)
        )

    weights = jnp.stack([weight_grad(gg_m, gg_o), weight_grad(ug_m, ug_o)]).astype(BF16)[None]
    token_grad = pl.pallas_call(
        combine_kernel,
        out_shape=jax.ShapeDtypeStruct((F, T), BF16),
        in_specs=vmem(4),
        out_specs=vmem(1)[0],
        name="combine",
    )(ret, ix, lg, router_weight.T)
    return token_grad.T, weights, router_sum.T


def solution(mesh):
    fine = Mesh(mesh.devices.reshape(ZL, X, CORE, Y, ZH), DP + EX)
    in_specs = (
        P(DP, EX),
        P(DP, EX),
        P(DP, EX),
        P(DP, None),
        P(DP, None),
        P(EX, None, DP, None),
        P(EX, DP, None),
        P(EX, None),
    )
    out_specs = (P(DP, EX), P(EX, None, DP, None), P(EX, None))
    return jax.shard_map(
        per_device, mesh=fine, in_specs=in_specs, out_specs=out_specs, check_vma=False
    )
```

```python
import jax
import jax.numpy as jnp
from jax import lax
from jax.experimental import pallas as pl
from jax.experimental.pallas import tpu as pltpu
from jax.sharding import Mesh, PartitionSpec as P


ZL, X, CORE, Y, ZH = 4, 4, 2, 8, 4
EX = ("y", "zh")
DP = ("zl", "x", "core")
E = 32
CAP = 10
T = 256
F = 64
D = 2048
KT = 2 * D // 128
AUX = 0.2
ROOT = 0.7978845608028654
CUBE = 0.044715
GROUPS = ZL * X
SENT = KT + KT // 4 + 1
BACK = KT // 2 + KT // 8
TILES = ZL * BACK + 4
HID = 160
BUNDLE = 3 * HID + 16
WIDE = D + 512
DISPATCH_KIB = 60000
CROSS = GROUPS * CAP + E
F32, BF16 = jnp.float32, jnp.bfloat16
CONTRACT_LAST = (((1,), (1,)), ((), ()))
CONTRACT_FIRST = (((0,), (0,)), ((), ()))


def vmem(n):
    return [pl.BlockSpec(memory_space=pltpu.VMEM)] * n


def iota(shape, dim):
    return lax.broadcasted_iota(jnp.int32, shape, dim)


def slots(idx):
    hit = iota((E, T), 0) == idx
    hot = jnp.where(hit, 1.0, 0.0).astype(F32)
    earlier = jnp.where(iota((T, T), 0) < iota((T, T), 1), 1.0, 0.0).astype(BF16)
    before = jnp.dot(hot.astype(BF16), earlier, preferred_element_type=F32)
    return hot, jnp.sum(hot * before, axis=0, keepdims=True)


def dispatch_kernel(tok_h, og_h, eo_h, pt_h, idx_h, out, tile, tok, og, eo, pt, ix, sems):
    copies = [
        pltpu.make_async_copy(a, b, sems.at[i])
        for i, (a, b) in enumerate(
            (
                (idx_h, ix),
                (tok_h, tok),
                (og_h, og),
                (pt_h, pt),
                (eo_h, eo),
            )
        )
    ]
    for c in copies:
        c.start()
    copies[0].wait()
    idx = ix[...]
    hot, slot = slots(idx)
    row = iota((E * 16, T), 0)
    sel = jnp.where(
        (lax.shift_right_logical(row, 4) == idx) & (lax.bitwise_and(row, 15) == slot.astype(jnp.int32)),
        1.0,
        0.0,
    ).astype(BF16)
    wide = jnp.where(iota((128, T), 0) == idx, 1.0, 0.0).astype(BF16)
    counts = lax.dot_general(jnp.ones((8, T), BF16), wide, CONTRACT_LAST, preferred_element_type=F32)
    tile[...] = counts.astype(BF16)
    for c in copies[1:]:
        c.wait()
    gate = jnp.sum(pt[...] * hot, axis=0, keepdims=True)
    grad = og[...].astype(F32)
    gated = (gate * grad).astype(BF16)
    dot = jnp.sum(grad * eo[...].astype(F32), axis=0, keepdims=True)
    both = jnp.concatenate([tok[...], gated], axis=0)
    sent = lax.dot_general(sel, both, CONTRACT_LAST, preferred_element_type=F32)
    h0 = dot.astype(BF16).astype(F32)
    h1 = (dot - h0).astype(BF16).astype(F32)
    h2 = dot - h0 - h1
    line = iota((16, 128), 0)
    extra = jnp.zeros((16, 128), F32)
    for i, h in enumerate((h0, h1, h2)):
        for j in range(2):
            extra = extra + jnp.where(line == CAP + 2 * i + j, h[:, 128 * j : 128 * (j + 1)], 0.0)
    out[...] = (sent.reshape(E, 16, 128) + extra[None]).astype(BF16)


def bundle_kernel(in_h, down_h, tile_h, out, tile, sems):
    copies = [
        pltpu.make_async_copy(a, b, sems.at[i])
        for i, (a, b) in enumerate(
            (
                (tile_h, tile),
                (in_h.at[0], out.at[pl.ds(0, HID)]),
                (in_h.at[1], out.at[pl.ds(HID, HID)]),
                (down_h, out.at[pl.ds(2 * HID, HID)]),
            )
        )
    ]
    for c in copies:
        c.start()
    out[3 * HID :, :] = jnp.zeros((BUNDLE - 3 * HID, D), BF16)
    copies[0].wait()
    out[3 * HID :, :128] = jnp.concatenate([tile[...], tile[...]], axis=0)
    for c in copies[1:]:
        c.wait()


def pack_kernel(got, tile, partner, out, dot_ref):
    low = iota((16, 128), 1) < F
    line = iota((8, 128), 0)
    tail = [jnp.zeros((8, 128), F32) for _ in range(KT // 4)]
    total = jnp.zeros((16, 128), F32)
    for j in range(E // 2):
        a = got[2 * j].astype(F32)
        b = got[2 * j + 1].astype(F32)
        total = total + a + b
        t = jnp.where(low, a, pltpu.roll(b, F, 1))
        g = jnp.where(low, pltpu.roll(a, F, 1), b)
        for k, v in ((j, t), (j + E // 2, g)):
            out[k] = v[:8].astype(BF16)
            i = k % 4
            rest = v[8:] if i == 0 else pltpu.roll(v[8:], 2 * i, 0)
            tail[k // 4] = jnp.where((line >= 2 * i) & (line < 2 * i + 2), rest, tail[k // 4])
    for m in range(KT // 4):
        out[KT + m] = tail[m].astype(BF16)
    pair = tile[...].astype(F32) + partner[3 * HID : 3 * HID + 8, :128].astype(F32)
    out[KT + KT // 4] = pair.astype(BF16)
    odd = lax.bitwise_and(line, 1)
    for h in range(2):
        pick = jnp.where((line >= 2) & (odd == h), total[8:], 0.0)
        dot_ref[:, 128 * h : 128 * (h + 1)] = jnp.sum(pick, axis=0, keepdims=True)


def spread():
    a, b = iota((128, 128), 0), iota((128, 128), 1)
    group = lax.bitwise_and(lax.shift_right_logical(a, 1), 15)
    want = 8 * group + 2 * lax.shift_right_logical(a, 5) + lax.bitwise_and(a, 1)
    return jnp.where(b == want, 1.0, 0.0)


def unpack(src, tok, dy):
    perm = spread().astype(BF16)
    for k in range(KT):
        dst, at = (tok, k) if k < KT // 2 else (dy, k - KT // 2)
        block = src[:, k].astype(F32).reshape(GROUPS * 8, 128).astype(BF16)
        dst[: GROUPS * 8, 128 * at : 128 * (at + 1)] = block
    for m in range(KT // 4):
        block = src[:, KT + m].astype(F32).reshape(GROUPS * 8, 128).astype(BF16)
        lines = jnp.dot(perm, block, preferred_element_type=F32).astype(BF16)
        for i in range(4):
            k = 4 * m + i
            dst, at = (tok, k) if k < KT // 2 else (dy, k - KT // 2)
            dst[GROUPS * 8 : GROUPS * CAP, 128 * at : 128 * (at + 1)] = lines[32 * i : 32 * (i + 1)]


def hidden_grads(tok, dy, w):
    rows = tok[:, :D]
    gate_pre = lax.dot_general(rows, w[:HID], CONTRACT_LAST, preferred_element_type=F32)
    up_pre = lax.dot_general(rows, w[HID : 2 * HID], CONTRACT_LAST, preferred_element_type=F32)
    hidden = lax.dot_general(dy[...], w[2 * HID : 3 * HID], CONTRACT_LAST, preferred_element_type=F32)
    square = gate_pre * gate_pre
    th = jnp.tanh(ROOT * (gate_pre + CUBE * square * gate_pre))
    half = 0.5 * (1.0 + th)
    slope = half + 0.5 * gate_pre * (1.0 - th * th) * (ROOT * (1.0 + 3.0 * CUBE * square))
    return (hidden * up_pre * slope).astype(BF16), (hidden * (gate_pre * half)).astype(BF16)


def split_lanes(v):
    high = v.astype(BF16).astype(F32)
    return jnp.where(iota(v.shape, 1) < F, high, v - high).astype(BF16)


def main_kernel(src, mine, other, dot_ref, pt_ref, idx_ref, tok_in, out, cross, gg_ref, ug_ref, lg_ref, dy):
    unpack(src, cross, dy)
    gg, ug = hidden_grads(cross, dy, mine)
    gg_o, ug_o = hidden_grads(cross, dy, other)
    gg_ref[...] = gg
    ug_ref[...] = ug
    cross[:, D : D + HID] = gg_o
    cross[:, D + 256 : D + 256 + HID] = ug_o
    perm = spread().astype(BF16)
    for m in range(KT // 8):
        cols = pl.ds(512 * m, 512)
        part = jnp.dot(gg, mine[:HID, cols], preferred_element_type=F32)
        part = part + jnp.dot(ug, mine[HID : 2 * HID, cols], preferred_element_type=F32)
        part = part + jnp.dot(gg_o, other[:HID, cols], preferred_element_type=F32)
        part = part + jnp.dot(ug_o, other[HID : 2 * HID, cols], preferred_element_type=F32)
        lines = []
        for i in range(4):
            block = part[:, 128 * i : 128 * (i + 1)]
            head = block[: GROUPS * 8].reshape(X, ZL, 8, 128).astype(BF16)
            for z in range(ZL):
                out[:, z * BACK + 4 * m + i] = head[:, z]
            lines.append(block[GROUPS * 8 :])
        tails = jnp.concatenate(lines, axis=0).astype(BF16)
        tails = lax.dot_general(perm, tails, CONTRACT_FIRST, preferred_element_type=F32)
        tails = tails.reshape(X, ZL, 8, 128).astype(BF16)
        for z in range(ZL):
            out[:, z * BACK + KT // 2 + m] = tails[:, z]
    count = jnp.sum(src[:, SENT - 1].astype(F32), axis=0)
    diagonal = iota((E, 128), 0) == iota((E, 128), 1)
    counts = jnp.sum(jnp.where(diagonal, count[:1], 0.0), axis=1, keepdims=True)
    pt = pt_ref[...]
    hot = jnp.where(iota((E, T), 0) == idx_ref[...], 1.0, 0.0)
    grad = hot * dot_ref[...] + AUX * E * counts / (T * E)
    lg = (pt * (grad - jnp.sum(pt * grad, axis=0, keepdims=True))).astype(BF16)
    lg_ref[...] = lg
    twice = jnp.concatenate([tok_in[...], tok_in[...]], axis=0)
    pair = split_lanes(lax.dot_general(lg, twice, CONTRACT_LAST, preferred_element_type=F32))
    for i in range(4):
        for x in range(X):
            out[x, ZL * BACK + i] = pair[8 * i : 8 * (i + 1)]


def merged(got, i):
    pair = jnp.sum(got[:, pl.ds(i, 4)].astype(F32), axis=0).reshape(E, 128)
    return pair + pltpu.roll(pair, F, 1)


def middle_kernel(got, out):
    for z in range(ZL):
        for k in range(BACK):
            out[z, k] = jnp.sum(got[:, z * BACK + k].astype(F32), axis=0).astype(BF16)
    pair = split_lanes(merged(got, ZL * BACK))
    for z in range(ZL):
        for i in range(4):
            out[z, BACK + i] = pair[8 * i : 8 * (i + 1)]


def sum_kernel(got, cross, out, bundle, router):
    low = iota((8, 128), 1) < F
    line = iota((8, 128), 0)

    def total(k):
        return jnp.sum(got[:, k].astype(F32), axis=0)

    for m in range(KT // 8):
        tail = total(KT // 2 + m)
        for i in range(4):
            k = 4 * m + i
            head = total(k)
            rest = tail if i == 0 else pltpu.roll(tail, 8 - 2 * i, 0)
            rest = jnp.where(line < 2, rest, 0.0)
            out[2 * k] = jnp.where(low, head, pltpu.roll(rest, F, 1)).astype(BF16)
            out[2 * k + 1] = jnp.where(low, pltpu.roll(head, F, 1), rest).astype(BF16)
    share = merged(got, BACK)
    router[...] = share
    bundle[: GROUPS * CAP, :] = cross[...]
    bundle[GROUPS * CAP :, :] = jnp.zeros((E, WIDE), BF16)
    bundle[GROUPS * CAP :, :128] = split_lanes(share)


def weight_kernel(mine, came, gg, ug, share, out, router):
    n = GROUPS * CAP
    for i, m in enumerate((gg, ug)):
        o = came[:n, D + 256 * i : D + 256 * i + HID]
        for c in range(D // 512):
            cols = pl.ds(512 * c, 512)
            grad = lax.dot_general(m[...], mine[:n, cols], CONTRACT_FIRST, preferred_element_type=F32)
            grad = grad + lax.dot_general(o, came[:n, cols], CONTRACT_FIRST, preferred_element_type=F32)
            out[i, :, cols] = grad.astype(BF16)
    pair = came[n:, :128].astype(F32)
    router[...] = (share[...] + pair + pltpu.roll(pair, F, 1))[:, :F]


def combine_kernel(ret, idx_ref, lg, rw, out):
    idx = idx_ref[...]
    _, slot = slots(idx)
    slot = slot.astype(jnp.int32)
    row = iota((E * 8, T), 0)
    mine = lax.shift_right_logical(row, 3) == idx
    c = lax.bitwise_and(row, 7)
    r = ret[...].reshape(E * 8, 128)
    acc = lax.dot_general(rw[...], lg[...], CONTRACT_FIRST, preferred_element_type=F32)
    for h in range(2):
        sel = jnp.where(mine & (c + 8 * h == slot), 1.0, 0.0).astype(BF16)
        p = lax.dot_general(r, sel, CONTRACT_FIRST, preferred_element_type=F32)
        acc = acc + p[F * h : F * (h + 1)]
    out[...] = acc.astype(BF16)


def local(kernel, outs, ins, flops, scratch=(), hbm=False, kib=8192):
    one = not isinstance(outs, tuple)
    return pl.pallas_call(
        kernel,
        out_shape=outs,
        in_specs=[pl.BlockSpec(memory_space=pltpu.HBM)] * len(ins) if hbm else vmem(len(ins)),
        out_specs=vmem(1)[0] if one else tuple(vmem(len(outs))),
        scratch_shapes=list(scratch),
        cost_estimate=pl.CostEstimate(flops=flops, bytes_accessed=0, transcendentals=0),
        compiler_params=pltpu.CompilerParams(vmem_limit_bytes=kib * 1024),
    )(*ins)


def shape(*dims, dtype=BF16):
    return jax.ShapeDtypeStruct(dims, dtype)


def per_device(tokens, out_grad, expert_out, probs, idx, in_weight, down_weight, router_weight):
    return layer(
        tokens.T,
        out_grad.T,
        expert_out.T,
        probs.T,
        idx.T,
        in_weight,
        down_weight,
        router_weight,
    )


def layer(tok, og, eo, pt, ix, in_weight, down_weight, router_weight):
    swap = [(0, 1), (1, 0)]
    send, tile = local(
        dispatch_kernel,
        (shape(E, 16, 128), shape(8, 128)),
        (tok, og, eo, pt, ix),
        10**7,
        (
            pltpu.VMEM((F, T), BF16),
            pltpu.VMEM((F, T), BF16),
            pltpu.VMEM((F, T), BF16),
            pltpu.VMEM((E, T), F32),
            pltpu.VMEM((1, T), jnp.int32),
            pltpu.SemaphoreType.DMA((5,)),
        ),
        hbm=True,
        kib=DISPATCH_KIB,
    )
    got = lax.all_to_all(send, EX, 0, 0, tiled=True)
    mine = local(
        bundle_kernel,
        shape(BUNDLE, D),
        (in_weight[0], down_weight[0], tile),
        10**6,
        (pltpu.VMEM((8, 128), BF16), pltpu.SemaphoreType.DMA((4,))),
        hbm=True,
        kib=60000,
    )
    other = lax.ppermute(mine, "core", swap)
    packed, gate_dot = local(pack_kernel, (shape(SENT, 8, 128), shape(1, T, dtype=F32)), (got, tile, other), 10**7)
    line = lax.all_to_all(jnp.broadcast_to(packed, (ZL, *packed.shape)), "zl", 0, 0, tiled=True)
    plane = lax.all_to_all(jnp.broadcast_to(line, (X, *line.shape)), "x", 0, 0, tiled=True)
    own = plane.reshape(GROUPS, SENT, 8, 128)
    rows = GROUPS * CAP
    work = 10 * rows * HID * D
    back, cross, gg, ug, lg = local(
        main_kernel,
        (shape(X, TILES, 8, 128), shape(rows, WIDE), shape(rows, HID), shape(rows, HID), shape(E, T)),
        (own, mine, other, gate_dot, pt, ix, tok),
        2 * work,
        (pltpu.VMEM((rows, D), BF16),),
        kib=20000,
    )
    landed = lax.all_to_all(back, "x", 0, 0, tiled=True)
    onward = local(middle_kernel, shape(ZL, BACK + 4, 8, 128), (landed,), 10**6)
    landed = lax.all_to_all(onward, "zl", 0, 0, tiled=True)
    rows_back, bundle, share = local(
        sum_kernel, (shape(E, 8, 128), shape(CROSS, WIDE), shape(E, 128, dtype=F32)), (landed, cross), 10**6
    )
    ret = lax.all_to_all(rows_back, EX, 0, 0, tiled=True)
    came = lax.ppermute(bundle, "core", swap)
    weights, router_sum = local(
        weight_kernel, (shape(2, HID, D), shape(E, F, dtype=F32)), (bundle, came, gg, ug, share), work, kib=12000
    )
    token_grad = local(combine_kernel, shape(F, T), (ret, ix, lg, router_weight.T), 10**7)
    return token_grad.T, weights[None], router_sum.T


def solution(mesh):
    fine = Mesh(mesh.devices.reshape(ZL, X, CORE, Y, ZH), DP + EX)
    in_specs = (
        P(DP, EX),
        P(DP, EX),
        P(DP, EX),
        P(DP, None),
        P(DP, None),
        P(EX, None, DP, None),
        P(EX, DP, None),
        P(EX, None),
    )
    out_specs = (P(DP, EX), P(EX, None, DP, None), P(EX, None))
    return jax.shard_map(
        per_device, mesh=fine, in_specs=in_specs, out_specs=out_specs, check_vma=False
    )
```

```python
import jax
import jax.numpy as jnp
from jax import lax
from jax.experimental import pallas as pl
from jax.experimental.pallas import tpu as pltpu
from jax.sharding import Mesh, PartitionSpec as P


ZL, X, CORE, Y, ZH = 4, 4, 2, 8, 4
EX = ("y", "zh")
DP = ("zl", "x", "core")
E = 32
CAP = 10
T = 256
F = 64
D = 2048
KT = 2 * D // 128
AUX = 0.2
ROOT = 0.7978845608028654
CUBE = 0.044715
GROUPS = ZL * X
SENT = KT + KT // 4 + 1
BACK = KT // 2 + KT // 8
TILES = ZL * BACK + 4
HID = 160
BUNDLE = 3 * HID + 16
WIDE = D + 512
DISPATCH_KIB = 60000
CROSS = GROUPS * CAP + E
F32, BF16 = jnp.float32, jnp.bfloat16
CONTRACT_LAST = (((1,), (1,)), ((), ()))
CONTRACT_FIRST = (((0,), (0,)), ((), ()))


def vmem(n):
    return [pl.BlockSpec(memory_space=pltpu.VMEM)] * n


def iota(shape, dim):
    return lax.broadcasted_iota(jnp.int32, shape, dim)


def slots(idx):
    hit = iota((E, T), 0) == idx
    hot = jnp.where(hit, 1.0, 0.0).astype(F32)
    earlier = jnp.where(iota((T, T), 0) < iota((T, T), 1), 1.0, 0.0).astype(BF16)
    before = jnp.dot(hot.astype(BF16), earlier, preferred_element_type=F32)
    return hot, jnp.sum(hot * before, axis=0, keepdims=True)


def dispatch_kernel(tok_h, og_h, eo_h, pt_h, idx_h, out, tile, tok, og, eo, pt, ix, sems):
    copies = [
        pltpu.make_async_copy(a, b, sems.at[i])
        for i, (a, b) in enumerate(
            (
                (idx_h, ix),
                (tok_h, tok),
                (og_h, og),
                (pt_h, pt),
                (eo_h, eo),
            )
        )
    ]
    for c in copies:
        c.start()
    copies[0].wait()
    idx = ix[...]
    hot, slot = slots(idx)
    row = iota((E * 16, T), 0)
    sel = jnp.where(
        (lax.shift_right_logical(row, 4) == idx) & (lax.bitwise_and(row, 15) == slot.astype(jnp.int32)),
        1.0,
        0.0,
    ).astype(BF16)
    wide = jnp.where(iota((128, T), 0) == idx, 1.0, 0.0).astype(BF16)
    counts = lax.dot_general(jnp.ones((8, T), BF16), wide, CONTRACT_LAST, preferred_element_type=F32)
    tile[...] = counts.astype(BF16)
    for c in copies[1:]:
        c.wait()
    gate = jnp.sum(pt[...] * hot, axis=0, keepdims=True)
    grad = og[...].astype(F32)
    gated = (gate * grad).astype(BF16)
    dot = jnp.sum(grad * eo[...].astype(F32), axis=0, keepdims=True)
    both = jnp.concatenate([tok[...], gated], axis=0)
    sent = lax.dot_general(sel, both, CONTRACT_LAST, preferred_element_type=F32)
    h0 = dot.astype(BF16).astype(F32)
    h1 = (dot - h0).astype(BF16).astype(F32)
    h2 = dot - h0 - h1
    line = iota((16, 128), 0)
    extra = jnp.zeros((16, 128), F32)
    for i, h in enumerate((h0, h1, h2)):
        for j in range(2):
            extra = extra + jnp.where(line == CAP + 2 * i + j, h[:, 128 * j : 128 * (j + 1)], 0.0)
    out[...] = (sent.reshape(E, 16, 128) + extra[None]).astype(BF16)


def bundle_kernel(in_h, down_h, tile_h, out, tile, sems):
    copies = [
        pltpu.make_async_copy(a, b, sems.at[i])
        for i, (a, b) in enumerate(
            (
                (tile_h, tile),
                (in_h.at[0], out.at[pl.ds(0, HID)]),
                (in_h.at[1], out.at[pl.ds(HID, HID)]),
                (down_h, out.at[pl.ds(2 * HID, HID)]),
            )
        )
    ]
    for c in copies:
        c.start()
    out[3 * HID :, :] = jnp.zeros((BUNDLE - 3 * HID, D), BF16)
    copies[0].wait()
    out[3 * HID :, :128] = jnp.concatenate([tile[...], tile[...]], axis=0)
    for c in copies[1:]:
        c.wait()


def pack_kernel(got, tile, partner, out, dot_ref):
    low = iota((16, 128), 1) < F
    line = iota((8, 128), 0)
    tail = [jnp.zeros((8, 128), F32) for _ in range(KT // 4)]
    total = jnp.zeros((16, 128), F32)
    for j in range(E // 2):
        a = got[2 * j].astype(F32)
        b = got[2 * j + 1].astype(F32)
        total = total + a + b
        t = jnp.where(low, a, pltpu.roll(b, F, 1))
        g = jnp.where(low, pltpu.roll(a, F, 1), b)
        for k, v in ((j, t), (j + E // 2, g)):
            out[k] = v[:8].astype(BF16)
            i = k % 4
            rest = v[8:] if i == 0 else pltpu.roll(v[8:], 2 * i, 0)
            tail[k // 4] = jnp.where((line >= 2 * i) & (line < 2 * i + 2), rest, tail[k // 4])
    for m in range(KT // 4):
        out[KT + m] = tail[m].astype(BF16)
    pair = tile[...].astype(F32) + partner[3 * HID : 3 * HID + 8, :128].astype(F32)
    out[KT + KT // 4] = pair.astype(BF16)
    odd = lax.bitwise_and(line, 1)
    for h in range(2):
        pick = jnp.where((line >= 2) & (odd == h), total[8:], 0.0)
        dot_ref[:, 128 * h : 128 * (h + 1)] = jnp.sum(pick, axis=0, keepdims=True)


def spread():
    a, b = iota((128, 128), 0), iota((128, 128), 1)
    group = lax.bitwise_and(lax.shift_right_logical(a, 1), 15)
    want = 8 * group + 2 * lax.shift_right_logical(a, 5) + lax.bitwise_and(a, 1)
    return jnp.where(b == want, 1.0, 0.0)


def unpack(src, tok, dy):
    perm = spread().astype(BF16)
    for k in range(KT):
        dst, at = (tok, k) if k < KT // 2 else (dy, k - KT // 2)
        block = src[:, k].astype(F32).reshape(GROUPS * 8, 128).astype(BF16)
        dst[: GROUPS * 8, 128 * at : 128 * (at + 1)] = block
    for m in range(KT // 4):
        block = src[:, KT + m].astype(F32).reshape(GROUPS * 8, 128).astype(BF16)
        lines = jnp.dot(perm, block, preferred_element_type=F32).astype(BF16)
        for i in range(4):
            k = 4 * m + i
            dst, at = (tok, k) if k < KT // 2 else (dy, k - KT // 2)
            dst[GROUPS * 8 : GROUPS * CAP, 128 * at : 128 * (at + 1)] = lines[32 * i : 32 * (i + 1)]


def hidden_grads(tok, dy, w):
    rows = tok[:, :D]
    gate_pre = lax.dot_general(rows, w[:HID], CONTRACT_LAST, preferred_element_type=F32)
    up_pre = lax.dot_general(rows, w[HID : 2 * HID], CONTRACT_LAST, preferred_element_type=F32)
    hidden = lax.dot_general(dy[...], w[2 * HID : 3 * HID], CONTRACT_LAST, preferred_element_type=F32)
    square = gate_pre * gate_pre
    th = jnp.tanh(ROOT * (gate_pre + CUBE * square * gate_pre))
    half = 0.5 * (1.0 + th)
    slope = half + 0.5 * gate_pre * (1.0 - th * th) * (ROOT * (1.0 + 3.0 * CUBE * square))
    return (hidden * up_pre * slope).astype(BF16), (hidden * (gate_pre * half)).astype(BF16)


def split_lanes(v):
    high = v.astype(BF16).astype(F32)
    return jnp.where(iota(v.shape, 1) < F, high, v - high).astype(BF16)


def main_kernel(src, mine, other, dot_ref, pt_ref, idx_ref, tok_in, out, cross, gg_ref, ug_ref, lg_ref, dy):
    unpack(src, cross, dy)
    gg, ug = hidden_grads(cross, dy, mine)
    gg_o, ug_o = hidden_grads(cross, dy, other)
    gg_ref[...] = gg
    ug_ref[...] = ug
    cross[:, D : D + HID] = gg_o
    cross[:, D + 256 : D + 256 + HID] = ug_o
    perm = spread().astype(BF16)
    for m in range(KT // 8):
        cols = pl.ds(512 * m, 512)
        part = jnp.dot(gg, mine[:HID, cols], preferred_element_type=F32)
        part = part + jnp.dot(ug, mine[HID : 2 * HID, cols], preferred_element_type=F32)
        part = part + jnp.dot(gg_o, other[:HID, cols], preferred_element_type=F32)
        part = part + jnp.dot(ug_o, other[HID : 2 * HID, cols], preferred_element_type=F32)
        lines = []
        for i in range(4):
            block = part[:, 128 * i : 128 * (i + 1)]
            head = block[: GROUPS * 8].reshape(X, ZL, 8, 128).astype(BF16)
            for z in range(ZL):
                out[:, z * BACK + 4 * m + i] = head[:, z]
            lines.append(block[GROUPS * 8 :])
        tails = jnp.concatenate(lines, axis=0).astype(BF16)
        tails = lax.dot_general(perm, tails, CONTRACT_FIRST, preferred_element_type=F32)
        tails = tails.reshape(X, ZL, 8, 128).astype(BF16)
        for z in range(ZL):
            out[:, z * BACK + KT // 2 + m] = tails[:, z]
    count = jnp.sum(src[:, SENT - 1].astype(F32), axis=0)
    diagonal = iota((E, 128), 0) == iota((E, 128), 1)
    counts = jnp.sum(jnp.where(diagonal, count[:1], 0.0), axis=1, keepdims=True)
    pt = pt_ref[...]
    hot = jnp.where(iota((E, T), 0) == idx_ref[...], 1.0, 0.0)
    grad = hot * dot_ref[...] + AUX * E * counts / (T * E)
    lg = (pt * (grad - jnp.sum(pt * grad, axis=0, keepdims=True))).astype(BF16)
    lg_ref[...] = lg
    twice = jnp.concatenate([tok_in[...], tok_in[...]], axis=0)
    pair = split_lanes(lax.dot_general(lg, twice, CONTRACT_LAST, preferred_element_type=F32))
    for i in range(4):
        for x in range(X):
            out[x, ZL * BACK + i] = pair[8 * i : 8 * (i + 1)]


def merged(got, i):
    pair = jnp.sum(got[:, pl.ds(i, 4)].astype(F32), axis=0).reshape(E, 128)
    return pair + pltpu.roll(pair, F, 1)


def middle_kernel(got, cross, out, bundle, share_ref):
    low = iota((8, 128), 1) < F
    line = iota((8, 128), 0)
    for z in range(ZL):

        def total(k):
            return jnp.sum(got[:, z * BACK + k].astype(F32), axis=0)

        for m in range(KT // 8):
            tail = total(KT // 2 + m)
            for i in range(4):
                k = 4 * m + i
                head = total(k)
                rest = tail if i == 0 else pltpu.roll(tail, 8 - 2 * i, 0)
                rest = jnp.where(line < 2, rest, 0.0)
                out[E * z + 2 * k] = jnp.where(low, head, pltpu.roll(rest, F, 1)).astype(BF16)
                out[E * z + 2 * k + 1] = jnp.where(low, pltpu.roll(head, F, 1), rest).astype(BF16)
    share = merged(got, ZL * BACK)
    share_ref[...] = share
    bundle[: GROUPS * CAP, :] = cross[...]
    bundle[GROUPS * CAP :, :] = jnp.zeros((E, WIDE), BF16)
    bundle[GROUPS * CAP :, :128] = split_lanes(share)


def weight_kernel(mine, came, gg, ug, out):
    n = GROUPS * CAP
    for i, m in enumerate((gg, ug)):
        o = came[:n, D + 256 * i : D + 256 * i + HID]
        for c in range(D // 512):
            cols = pl.ds(512 * c, 512)
            grad = lax.dot_general(m[...], mine[:n, cols], CONTRACT_FIRST, preferred_element_type=F32)
            grad = grad + lax.dot_general(o, came[:n, cols], CONTRACT_FIRST, preferred_element_type=F32)
            out[i, :, cols] = grad.astype(BF16)


def folded(a, b):
    pair = a.astype(F32) + b.astype(F32)
    return pair + pltpu.roll(pair, F, 1)


def cores_kernel(share, came, out):
    out[...] = split_lanes(share[...] + folded(came[GROUPS * CAP :, :128], jnp.zeros((E, 128), F32)))


def pairs_kernel(a, b, out):
    out[...] = split_lanes(folded(a[...], b[...]))


def router_kernel(a, b, out):
    out[...] = folded(a[...], b[...])[:, :F]


def combine_kernel(ret, idx_ref, lg, rw, out):
    idx = idx_ref[...]
    _, slot = slots(idx)
    slot = slot.astype(jnp.int32)
    row = iota((E * 8, T), 0)
    mine = lax.shift_right_logical(row, 3) == idx
    c = lax.bitwise_and(row, 7)
    r = ret[pl.ds(0, E)].astype(F32)
    for z in range(1, ZL):
        r = r + ret[pl.ds(E * z, E)].astype(F32)
    high = r.astype(BF16)
    low = (r - high.astype(F32)).astype(BF16)
    acc = lax.dot_general(rw[...], lg[...], CONTRACT_FIRST, preferred_element_type=F32)
    for h in range(2):
        sel = jnp.where(mine & (c + 8 * h == slot), 1.0, 0.0).astype(BF16)
        for part in (high, low):
            lanes = part.reshape(E * 8, 128)
            p = lax.dot_general(lanes, sel, CONTRACT_FIRST, preferred_element_type=F32)
            acc = acc + p[F * h : F * (h + 1)]
    out[...] = acc.astype(BF16)


def local(kernel, outs, ins, flops, scratch=(), hbm=False, kib=8192):
    one = not isinstance(outs, tuple)
    return pl.pallas_call(
        kernel,
        out_shape=outs,
        in_specs=[pl.BlockSpec(memory_space=pltpu.HBM)] * len(ins) if hbm else vmem(len(ins)),
        out_specs=vmem(1)[0] if one else tuple(vmem(len(outs))),
        scratch_shapes=list(scratch),
        cost_estimate=pl.CostEstimate(flops=flops, bytes_accessed=0, transcendentals=0),
        compiler_params=pltpu.CompilerParams(vmem_limit_bytes=kib * 1024),
    )(*ins)


def shape(*dims, dtype=BF16):
    return jax.ShapeDtypeStruct(dims, dtype)


def per_device(tokens, out_grad, expert_out, probs, idx, in_weight, down_weight, router_weight):
    return layer(
        tokens.T,
        out_grad.T,
        expert_out.T,
        probs.T,
        idx.T,
        in_weight,
        down_weight,
        router_weight,
    )


def layer(tok, og, eo, pt, ix, in_weight, down_weight, router_weight):
    swap = [(0, 1), (1, 0)]
    send, tile = local(
        dispatch_kernel,
        (shape(E, 16, 128), shape(8, 128)),
        (tok, og, eo, pt, ix),
        10**7,
        (
            pltpu.VMEM((F, T), BF16),
            pltpu.VMEM((F, T), BF16),
            pltpu.VMEM((F, T), BF16),
            pltpu.VMEM((E, T), F32),
            pltpu.VMEM((1, T), jnp.int32),
            pltpu.SemaphoreType.DMA((5,)),
        ),
        hbm=True,
        kib=DISPATCH_KIB,
    )
    got = lax.all_to_all(send, EX, 0, 0, tiled=True)
    mine = local(
        bundle_kernel,
        shape(BUNDLE, D),
        (in_weight[0], down_weight[0], tile),
        10**6,
        (pltpu.VMEM((8, 128), BF16), pltpu.SemaphoreType.DMA((4,))),
        hbm=True,
        kib=60000,
    )
    other = lax.ppermute(mine, "core", swap)
    packed, gate_dot = local(pack_kernel, (shape(SENT, 8, 128), shape(1, T, dtype=F32)), (got, tile, other), 10**7)
    line = lax.all_to_all(jnp.broadcast_to(packed, (ZL, *packed.shape)), "zl", 0, 0, tiled=True)
    plane = lax.all_to_all(jnp.broadcast_to(line, (X, *line.shape)), "x", 0, 0, tiled=True)
    own = plane.reshape(GROUPS, SENT, 8, 128)
    rows = GROUPS * CAP
    work = 10 * rows * HID * D
    back, cross, gg, ug, lg = local(
        main_kernel,
        (shape(X, TILES, 8, 128), shape(rows, WIDE), shape(rows, HID), shape(rows, HID), shape(E, T)),
        (own, mine, other, gate_dot, pt, ix, tok),
        2 * work,
        (pltpu.VMEM((rows, D), BF16),),
        kib=20000,
    )
    landed = lax.all_to_all(back, "x", 0, 0, tiled=True)
    rows_back, bundle, share = local(
        middle_kernel, (shape(ZL * E, 8, 128), shape(CROSS, WIDE), shape(E, 128, dtype=F32)), (landed, cross), 10**6
    )
    ret = lax.all_to_all(rows_back, ("zl", *EX), 0, 0, tiled=True)
    came = lax.ppermute(bundle, "core", swap)
    pair = local(cores_kernel, shape(E, 128), (share, came), 10**5)
    got = lax.ppermute(pair, "zl", [(0, 1), (1, 0), (2, 3), (3, 2)])
    weights = local(weight_kernel, shape(2, HID, D), (bundle, came, gg, ug), work, kib=12000)
    pair = local(pairs_kernel, shape(E, 128), (pair, got), 10**5)
    got = lax.ppermute(pair, "zl", [(0, 2), (2, 0), (1, 3), (3, 1)])
    token_grad = local(combine_kernel, shape(F, T), (ret, ix, lg, router_weight.T), 10**7)
    router_sum = local(router_kernel, shape(E, F, dtype=F32), (pair, got), 10**5)
    return token_grad.T, weights[None], router_sum.T


def solution(mesh):
    fine = Mesh(mesh.devices.reshape(ZL, X, CORE, Y, ZH), DP + EX)
    in_specs = (
        P(DP, EX),
        P(DP, EX),
        P(DP, EX),
        P(DP, None),
        P(DP, None),
        P(EX, None, DP, None),
        P(EX, DP, None),
        P(EX, None),
    )
    out_specs = (P(DP, EX), P(EX, None, DP, None), P(EX, None))
    return jax.shard_map(
        per_device, mesh=fine, in_specs=in_specs, out_specs=out_specs, check_vma=False
    )
```

```python
import jax
import jax.numpy as jnp
from jax import lax
from jax.experimental import pallas as pl
from jax.experimental.pallas import tpu as pltpu
from jax.sharding import Mesh, PartitionSpec as P


ZL, X, CORE = 4, 4, 2
EX = "expert"
DP = ("zl", "x", "core")
E = 32
CAP = 10
T = 256
F = 64
D = 2048
KT = 2 * D // 128
AUX = 0.2
ROOT = 0.7978845608028654
CUBE = 0.044715
GROUPS = ZL * X
SENT = KT + KT // 4 + 1
BACK = KT // 2 + KT // 8
TILES = ZL * BACK + 4
HID = 160
BUNDLE = 3 * HID + 16
WIDE = D + 512
FROM_LAST = list(range(E))[::-1]
DISPATCH_KIB = 60000
CROSS = GROUPS * CAP + E
F32, BF16 = jnp.float32, jnp.bfloat16
CONTRACT_LAST = (((1,), (1,)), ((), ()))
CONTRACT_FIRST = (((0,), (0,)), ((), ()))


def vmem(n):
    return [pl.BlockSpec(memory_space=pltpu.VMEM)] * n


def iota(shape, dim):
    return lax.broadcasted_iota(jnp.int32, shape, dim)


def slots(idx):
    hit = iota((E, T), 0) == idx
    hot = jnp.where(hit, 1.0, 0.0).astype(F32)
    earlier = jnp.where(iota((T, T), 0) < iota((T, T), 1), 1.0, 0.0).astype(BF16)
    before = jnp.dot(hot.astype(BF16), earlier, preferred_element_type=F32)
    return hot, jnp.sum(hot * before, axis=0, keepdims=True)


def dispatch_kernel(tok_h, og_h, eo_h, pt_h, idx_h, out, tile, tok, og, eo, pt, ix, sems):
    copies = [
        pltpu.make_async_copy(a, b, sems.at[i])
        for i, (a, b) in enumerate(
            (
                (idx_h, ix),
                (tok_h, tok),
                (og_h, og),
                (pt_h, pt),
                (eo_h, eo),
            )
        )
    ]
    for c in copies:
        c.start()
    copies[0].wait()
    idx = ix[...]
    hot, slot = slots(idx)
    row = iota((E * 16, T), 0)
    sel = jnp.where(
        (E - 1 - lax.shift_right_logical(row, 4) == idx)
        & (lax.bitwise_and(row, 15) == slot.astype(jnp.int32)),
        1.0,
        0.0,
    ).astype(BF16)
    wide = jnp.where(iota((128, T), 0) == idx, 1.0, 0.0).astype(BF16)
    counts = lax.dot_general(jnp.ones((8, T), BF16), wide, CONTRACT_LAST, preferred_element_type=F32)
    tile[...] = counts.astype(BF16)
    for c in copies[1:]:
        c.wait()
    gate = jnp.sum(pt[...] * hot, axis=0, keepdims=True)
    grad = og[...].astype(F32)
    gated = (gate * grad).astype(BF16)
    dot = jnp.sum(grad * eo[...].astype(F32), axis=0, keepdims=True)
    both = jnp.concatenate([tok[...], gated], axis=0)
    sent = lax.dot_general(sel, both, CONTRACT_LAST, preferred_element_type=F32)
    h0 = dot.astype(BF16).astype(F32)
    h1 = (dot - h0).astype(BF16).astype(F32)
    h2 = dot - h0 - h1
    line = iota((16, 128), 0)
    extra = jnp.zeros((16, 128), F32)
    for i, h in enumerate((h0, h1, h2)):
        for j in range(2):
            extra = extra + jnp.where(line == CAP + 2 * i + j, h[:, 128 * j : 128 * (j + 1)], 0.0)
    out[...] = (sent.reshape(E, 16, 128) + extra[None]).astype(BF16)


def bundle_kernel(in_h, down_h, tile_h, out, tile, sems):
    copies = [
        pltpu.make_async_copy(a, b, sems.at[i])
        for i, (a, b) in enumerate(
            (
                (tile_h, tile),
                (in_h.at[0], out.at[pl.ds(0, HID)]),
                (in_h.at[1], out.at[pl.ds(HID, HID)]),
                (down_h, out.at[pl.ds(2 * HID, HID)]),
            )
        )
    ]
    for c in copies:
        c.start()
    out[3 * HID :, :] = jnp.zeros((BUNDLE - 3 * HID, D), BF16)
    copies[0].wait()
    out[3 * HID :, :128] = jnp.concatenate([tile[...], tile[...]], axis=0)
    for c in copies[1:]:
        c.wait()


def pack_kernel(got, tile, partner, out, dot_ref):
    low = iota((16, 128), 1) < F
    line = iota((8, 128), 0)
    tail = [jnp.zeros((8, 128), F32) for _ in range(KT // 4)]
    total = jnp.zeros((16, 128), F32)
    for j in range(E // 2):
        a = got[E - 1 - 2 * j].astype(F32)
        b = got[E - 2 - 2 * j].astype(F32)
        total = total + a + b
        t = jnp.where(low, a, pltpu.roll(b, F, 1))
        g = jnp.where(low, pltpu.roll(a, F, 1), b)
        for k, v in ((j, t), (j + E // 2, g)):
            out[k] = v[:8].astype(BF16)
            i = k % 4
            rest = v[8:] if i == 0 else pltpu.roll(v[8:], 2 * i, 0)
            tail[k // 4] = jnp.where((line >= 2 * i) & (line < 2 * i + 2), rest, tail[k // 4])
    for m in range(KT // 4):
        out[KT + m] = tail[m].astype(BF16)
    pair = tile[...].astype(F32) + partner[3 * HID : 3 * HID + 8, :128].astype(F32)
    out[KT + KT // 4] = pair.astype(BF16)
    odd = lax.bitwise_and(line, 1)
    for h in range(2):
        pick = jnp.where((line >= 2) & (odd == h), total[8:], 0.0)
        dot_ref[:, 128 * h : 128 * (h + 1)] = jnp.sum(pick, axis=0, keepdims=True)


def spread():
    a, b = iota((128, 128), 0), iota((128, 128), 1)
    group = lax.bitwise_and(lax.shift_right_logical(a, 1), 15)
    want = 8 * group + 2 * lax.shift_right_logical(a, 5) + lax.bitwise_and(a, 1)
    return jnp.where(b == want, 1.0, 0.0)


def unpack(src, tok, dy):
    perm = spread().astype(BF16)
    for k in range(KT):
        dst, at = (tok, k) if k < KT // 2 else (dy, k - KT // 2)
        block = src[:, k].astype(F32).reshape(GROUPS * 8, 128).astype(BF16)
        dst[: GROUPS * 8, 128 * at : 128 * (at + 1)] = block
    for m in range(KT // 4):
        block = src[:, KT + m].astype(F32).reshape(GROUPS * 8, 128).astype(BF16)
        lines = jnp.dot(perm, block, preferred_element_type=F32).astype(BF16)
        for i in range(4):
            k = 4 * m + i
            dst, at = (tok, k) if k < KT // 2 else (dy, k - KT // 2)
            dst[GROUPS * 8 : GROUPS * CAP, 128 * at : 128 * (at + 1)] = lines[32 * i : 32 * (i + 1)]


def hidden_grads(tok, dy, w):
    rows = tok[:, :D]
    gate_pre = lax.dot_general(rows, w[:HID], CONTRACT_LAST, preferred_element_type=F32)
    up_pre = lax.dot_general(rows, w[HID : 2 * HID], CONTRACT_LAST, preferred_element_type=F32)
    hidden = lax.dot_general(dy[...], w[2 * HID : 3 * HID], CONTRACT_LAST, preferred_element_type=F32)
    square = gate_pre * gate_pre
    th = jnp.tanh(ROOT * (gate_pre + CUBE * square * gate_pre))
    half = 0.5 * (1.0 + th)
    slope = half + 0.5 * gate_pre * (1.0 - th * th) * (ROOT * (1.0 + 3.0 * CUBE * square))
    return (hidden * up_pre * slope).astype(BF16), (hidden * (gate_pre * half)).astype(BF16)


def split_lanes(v):
    high = v.astype(BF16).astype(F32)
    return jnp.where(iota(v.shape, 1) < F, high, v - high).astype(BF16)


def main_kernel(src, mine, other, dot_ref, pt_ref, idx_ref, tok_in, out, cross, gg_ref, ug_ref, lg_ref, dy):
    unpack(src, cross, dy)
    gg, ug = hidden_grads(cross, dy, mine)
    gg_o, ug_o = hidden_grads(cross, dy, other)
    gg_ref[...] = gg
    ug_ref[...] = ug
    cross[:, D : D + HID] = gg_o
    cross[:, D + 256 : D + 256 + HID] = ug_o
    perm = spread().astype(BF16)
    for m in range(KT // 8):
        cols = pl.ds(512 * m, 512)
        part = jnp.dot(gg, mine[:HID, cols], preferred_element_type=F32)
        part = part + jnp.dot(ug, mine[HID : 2 * HID, cols], preferred_element_type=F32)
        part = part + jnp.dot(gg_o, other[:HID, cols], preferred_element_type=F32)
        part = part + jnp.dot(ug_o, other[HID : 2 * HID, cols], preferred_element_type=F32)
        lines = []
        for i in range(4):
            block = part[:, 128 * i : 128 * (i + 1)]
            head = block[: GROUPS * 8].reshape(X, ZL, 8, 128).astype(BF16)
            for z in range(ZL):
                out[:, z * BACK + 4 * m + i] = head[:, z]
            lines.append(block[GROUPS * 8 :])
        tails = jnp.concatenate(lines, axis=0).astype(BF16)
        tails = lax.dot_general(perm, tails, CONTRACT_FIRST, preferred_element_type=F32)
        tails = tails.reshape(X, ZL, 8, 128).astype(BF16)
        for z in range(ZL):
            out[:, z * BACK + KT // 2 + m] = tails[:, z]
    count = jnp.sum(src[:, SENT - 1].astype(F32), axis=0)
    diagonal = iota((E, 128), 0) == iota((E, 128), 1)
    counts = jnp.sum(jnp.where(diagonal, count[:1], 0.0), axis=1, keepdims=True)
    pt = pt_ref[...]
    hot = jnp.where(iota((E, T), 0) == idx_ref[...], 1.0, 0.0)
    grad = hot * dot_ref[...] + AUX * E * counts / (T * E)
    lg = (pt * (grad - jnp.sum(pt * grad, axis=0, keepdims=True))).astype(BF16)
    lg_ref[...] = lg
    twice = jnp.concatenate([tok_in[...], tok_in[...]], axis=0)
    pair = split_lanes(lax.dot_general(lg, twice, CONTRACT_LAST, preferred_element_type=F32))
    for i in range(4):
        for x in range(X):
            out[x, ZL * BACK + i] = pair[8 * i : 8 * (i + 1)]


def merged(got, i):
    pair = jnp.sum(got[:, pl.ds(i, 4)].astype(F32), axis=0).reshape(E, 128)
    return pair + pltpu.roll(pair, F, 1)


def middle_kernel(got, cross, out, bundle, share_ref):
    low = iota((8, 128), 1) < F
    line = iota((8, 128), 0)
    for z in range(ZL):

        def total(k):
            return jnp.sum(got[:, z * BACK + k].astype(F32), axis=0)

        for m in range(KT // 8):
            tail = total(KT // 2 + m)
            for i in range(4):
                k = 4 * m + i
                head = total(k)
                rest = tail if i == 0 else pltpu.roll(tail, 8 - 2 * i, 0)
                rest = jnp.where(line < 2, rest, 0.0)
                out[E * z + 2 * k] = jnp.where(low, head, pltpu.roll(rest, F, 1)).astype(BF16)
                out[E * z + 2 * k + 1] = jnp.where(low, pltpu.roll(head, F, 1), rest).astype(BF16)
    share = merged(got, ZL * BACK)
    share_ref[...] = share
    bundle[: GROUPS * CAP, :] = cross[...]
    bundle[GROUPS * CAP :, :] = jnp.zeros((E, WIDE), BF16)
    bundle[GROUPS * CAP :, :128] = split_lanes(share)


def weight_kernel(mine, came, gg, ug, out):
    n = GROUPS * CAP
    for i, m in enumerate((gg, ug)):
        o = came[:n, D + 256 * i : D + 256 * i + HID]
        for c in range(D // 512):
            cols = pl.ds(512 * c, 512)
            grad = lax.dot_general(m[...], mine[:n, cols], CONTRACT_FIRST, preferred_element_type=F32)
            grad = grad + lax.dot_general(o, came[:n, cols], CONTRACT_FIRST, preferred_element_type=F32)
            out[i, :, cols] = grad.astype(BF16)


def folded(a, b):
    pair = a.astype(F32) + b.astype(F32)
    return pair + pltpu.roll(pair, F, 1)


def cores_kernel(share, came, out):
    out[...] = split_lanes(share[...] + folded(came[GROUPS * CAP :, :128], jnp.zeros((E, 128), F32)))


def pairs_kernel(a, b, out):
    out[...] = split_lanes(folded(a[...], b[...]))


def combine_kernel(ret, idx_ref, lg, rw, pair, far, out, router):
    router[...] = folded(pair[...], far[...])[:, :F]
    idx = idx_ref[...]
    _, slot = slots(idx)
    slot = slot.astype(jnp.int32)
    row = iota((E * 8, T), 0)
    mine = lax.shift_right_logical(row, 3) == idx
    c = lax.bitwise_and(row, 7)
    r = ret[pl.ds(0, E)].astype(F32)
    for z in range(1, ZL):
        r = r + ret[pl.ds(E * z, E)].astype(F32)
    high = r.astype(BF16)
    low = (r - high.astype(F32)).astype(BF16)
    acc = lax.dot_general(rw[...], lg[...], CONTRACT_FIRST, preferred_element_type=F32)
    for h in range(2):
        sel = jnp.where(mine & (c + 8 * h == slot), 1.0, 0.0).astype(BF16)
        for part in (high, low):
            lanes = part.reshape(E * 8, 128)
            p = lax.dot_general(lanes, sel, CONTRACT_FIRST, preferred_element_type=F32)
            acc = acc + p[F * h : F * (h + 1)]
    out[...] = acc.astype(BF16)


def local(kernel, outs, ins, flops, scratch=(), hbm=False, kib=8192):
    one = not isinstance(outs, tuple)
    return pl.pallas_call(
        kernel,
        out_shape=outs,
        in_specs=[pl.BlockSpec(memory_space=pltpu.HBM)] * len(ins) if hbm else vmem(len(ins)),
        out_specs=vmem(1)[0] if one else tuple(vmem(len(outs))),
        scratch_shapes=list(scratch),
        cost_estimate=pl.CostEstimate(flops=flops, bytes_accessed=0, transcendentals=0),
        compiler_params=pltpu.CompilerParams(vmem_limit_bytes=kib * 1024),
    )(*ins)


def shape(*dims, dtype=BF16):
    return jax.ShapeDtypeStruct(dims, dtype)


def per_device(tokens, out_grad, expert_out, probs, idx, in_weight, down_weight, router_weight):
    return layer(
        tokens.T,
        out_grad.T,
        expert_out.T,
        probs.T,
        idx.T,
        in_weight,
        down_weight,
        router_weight,
    )


def layer(tok, og, eo, pt, ix, in_weight, down_weight, router_weight):
    swap = [(0, 1), (1, 0)]
    send, tile = local(
        dispatch_kernel,
        (shape(E, 16, 128), shape(8, 128)),
        (tok, og, eo, pt, ix),
        10**7,
        (
            pltpu.VMEM((F, T), BF16),
            pltpu.VMEM((F, T), BF16),
            pltpu.VMEM((F, T), BF16),
            pltpu.VMEM((E, T), F32),
            pltpu.VMEM((1, T), jnp.int32),
            pltpu.SemaphoreType.DMA((5,)),
        ),
        hbm=True,
        kib=DISPATCH_KIB,
    )
    got = lax.all_to_all(send, EX, 0, 0, tiled=True, axis_index_groups=[FROM_LAST])
    mine = local(
        bundle_kernel,
        shape(BUNDLE, D),
        (in_weight[0], down_weight[0], tile),
        10**6,
        (pltpu.VMEM((8, 128), BF16), pltpu.SemaphoreType.DMA((4,))),
        hbm=True,
        kib=60000,
    )
    other = lax.ppermute(mine, "core", swap)
    packed, gate_dot = local(pack_kernel, (shape(SENT, 8, 128), shape(1, T, dtype=F32)), (got, tile, other), 10**7)
    line = lax.all_to_all(jnp.broadcast_to(packed, (ZL, *packed.shape)), "zl", 0, 0, tiled=True)
    plane = lax.all_to_all(jnp.broadcast_to(line, (X, *line.shape)), "x", 0, 0, tiled=True)
    own = plane.reshape(GROUPS, SENT, 8, 128)
    rows = GROUPS * CAP
    work = 10 * rows * HID * D
    back, cross, gg, ug, lg = local(
        main_kernel,
        (shape(X, TILES, 8, 128), shape(rows, WIDE), shape(rows, HID), shape(rows, HID), shape(E, T)),
        (own, mine, other, gate_dot, pt, ix, tok),
        2 * work,
        (pltpu.VMEM((rows, D), BF16),),
        kib=20000,
    )
    landed = lax.all_to_all(back, "x", 0, 0, tiled=True)
    rows_back, bundle, share = local(
        middle_kernel, (shape(ZL * E, 8, 128), shape(CROSS, WIDE), shape(E, 128, dtype=F32)), (landed, cross), 10**6
    )
    ret = lax.all_to_all(rows_back, ("zl", EX), 0, 0, tiled=True)
    came = lax.ppermute(bundle, "core", swap)
    pair = local(cores_kernel, shape(E, 128), (share, came), 10**5)
    got = lax.ppermute(pair, "zl", [(0, 1), (1, 0), (2, 3), (3, 2)])
    weights = local(weight_kernel, shape(2, HID, D), (bundle, came, gg, ug), work, kib=12000)
    pair = local(pairs_kernel, shape(E, 128), (pair, got), 10**5)
    got = lax.ppermute(pair, "zl", [(0, 2), (2, 0), (1, 3), (3, 1)])
    token_grad, router_sum = local(
        combine_kernel, (shape(F, T), shape(E, F, dtype=F32)), (ret, ix, lg, router_weight.T, pair, got), 10**7
    )
    return token_grad.T, weights[None], router_sum.T


def solution(mesh):
    fine = Mesh(mesh.devices.reshape(ZL, X, CORE, E), (*DP, EX))
    in_specs = (
        P(DP, EX),
        P(DP, EX),
        P(DP, EX),
        P(DP, None),
        P(DP, None),
        P(EX, None, DP, None),
        P(EX, DP, None),
        P(EX, None),
    )
    out_specs = (P(DP, EX), P(EX, None, DP, None), P(EX, None))
    return jax.shard_map(
        per_device, mesh=fine, in_specs=in_specs, out_specs=out_specs, check_vma=False
    )
```

```python
import jax
import jax.numpy as jnp
from jax import lax
from jax.experimental import pallas as pl
from jax.experimental.pallas import tpu as pltpu
from jax.sharding import Mesh, PartitionSpec as P


ZL, X, CORE = 4, 4, 2
EX = "expert"
DP = ("zl", "x", "core")
E = 32
CAP = 10
T = 256
F = 64
D = 2048
KT = 2 * D // 128
AUX = 0.2
ROOT = 0.7978845608028654
CUBE = 0.044715
GROUPS = ZL * X
SENT = KT + KT // 4 + 1
BACK = KT // 2 + KT // 8
TILES = ZL * BACK + 4
HID = 160
BUNDLE = 3 * HID + 16
WIDE = D + 512
AWAY = [4 * y + z for y in (7, 6, 5, 4, 0, 1, 2, 3) for z in (3, 2, 0, 1)]
NEAR = [1, 0, 2, 3]
HOME = [
    E * (z % 4) + 4 * (y % 8) + z % 16 // 4
    for z in (*range(0, -8, -1), *range(1, 9))
    for y in (0, -1, -2, -3, 1, 2, 3, 4)
]
DISPATCH_KIB = 60000
CROSS = GROUPS * CAP + E
F32, BF16 = jnp.float32, jnp.bfloat16
CONTRACT_LAST = (((1,), (1,)), ((), ()))
CONTRACT_FIRST = (((0,), (0,)), ((), ()))


def vmem(n):
    return [pl.BlockSpec(memory_space=pltpu.VMEM)] * n


def iota(shape, dim):
    return lax.broadcasted_iota(jnp.int32, shape, dim)


def slots(idx):
    hit = iota((E, T), 0) == idx
    hot = jnp.where(hit, 1.0, 0.0).astype(F32)
    earlier = jnp.where(iota((T, T), 0) < iota((T, T), 1), 1.0, 0.0).astype(BF16)
    before = jnp.dot(hot.astype(BF16), earlier, preferred_element_type=F32)
    return hot, jnp.sum(hot * before, axis=0, keepdims=True)


def dispatch_kernel(tok_h, og_h, eo_h, pt_h, idx_h, out, tile, tok, og, eo, pt, ix, sems):
    copies = [
        pltpu.make_async_copy(a, b, sems.at[i])
        for i, (a, b) in enumerate(
            (
                (idx_h, ix),
                (tok_h, tok),
                (og_h, og),
                (pt_h, pt),
                (eo_h, eo),
            )
        )
    ]
    for c in copies:
        c.start()
    copies[0].wait()
    idx = ix[...]
    hot, slot = slots(idx)
    row = iota((E * 16, T), 0)
    y, z = lax.shift_right_logical(row, 6), lax.bitwise_and(lax.shift_right_logical(row, 4), 3)
    expert = 4 * jnp.where(y < 4, 7 - y, y - 4) + jnp.where(z < 2, 3 - z, z - 2)
    sel = jnp.where(
        (expert == idx)
        & (lax.bitwise_and(row, 15) == slot.astype(jnp.int32)),
        1.0,
        0.0,
    ).astype(BF16)
    wide = jnp.where(iota((128, T), 0) == idx, 1.0, 0.0).astype(BF16)
    counts = lax.dot_general(jnp.ones((8, T), BF16), wide, CONTRACT_LAST, preferred_element_type=F32)
    tile[...] = counts.astype(BF16)
    for c in copies[1:]:
        c.wait()
    gate = jnp.sum(pt[...] * hot, axis=0, keepdims=True)
    grad = og[...].astype(F32)
    gated = (gate * grad).astype(BF16)
    dot = jnp.sum(grad * eo[...].astype(F32), axis=0, keepdims=True)
    both = jnp.concatenate([tok[...], gated], axis=0)
    sent = lax.dot_general(sel, both, CONTRACT_LAST, preferred_element_type=F32)
    h0 = dot.astype(BF16).astype(F32)
    h1 = (dot - h0).astype(BF16).astype(F32)
    h2 = dot - h0 - h1
    line = iota((16, 128), 0)
    extra = jnp.zeros((16, 128), F32)
    for i, h in enumerate((h0, h1, h2)):
        for j in range(2):
            extra = extra + jnp.where(line == CAP + 2 * i + j, h[:, 128 * j : 128 * (j + 1)], 0.0)
    out[...] = (sent.reshape(E, 16, 128) + extra[None]).astype(BF16)


def bundle_kernel(in_h, down_h, tile_h, out, tile, sems):
    copies = [
        pltpu.make_async_copy(a, b, sems.at[i])
        for i, (a, b) in enumerate(
            (
                (tile_h, tile),
                (in_h.at[0], out.at[pl.ds(0, HID)]),
                (in_h.at[1], out.at[pl.ds(HID, HID)]),
                (down_h, out.at[pl.ds(2 * HID, HID)]),
            )
        )
    ]
    for c in copies:
        c.start()
    out[3 * HID :, :] = jnp.zeros((BUNDLE - 3 * HID, D), BF16)
    copies[0].wait()
    out[3 * HID :, :128] = jnp.concatenate([tile[...], tile[...]], axis=0)
    for c in copies[1:]:
        c.wait()


def pack_kernel(got, tile, partner, out, dot_ref):
    low = iota((16, 128), 1) < F
    line = iota((8, 128), 0)
    tail = [jnp.zeros((8, 128), F32) for _ in range(KT // 4)]
    total = jnp.zeros((16, 128), F32)
    for j in range(E // 2):
        a = got[AWAY.index(2 * j)].astype(F32)
        b = got[AWAY.index(2 * j + 1)].astype(F32)
        total = total + a + b
        t = jnp.where(low, a, pltpu.roll(b, F, 1))
        g = jnp.where(low, pltpu.roll(a, F, 1), b)
        for k, v in ((j, t), (j + E // 2, g)):
            out[k] = v[:8].astype(BF16)
            i = k % 4
            rest = v[8:] if i == 0 else pltpu.roll(v[8:], 2 * i, 0)
            tail[k // 4] = jnp.where((line >= 2 * i) & (line < 2 * i + 2), rest, tail[k // 4])
    for m in range(KT // 4):
        out[KT + m] = tail[m].astype(BF16)
    pair = tile[...].astype(F32) + partner[3 * HID : 3 * HID + 8, :128].astype(F32)
    out[KT + KT // 4] = pair.astype(BF16)
    odd = lax.bitwise_and(line, 1)
    for h in range(2):
        pick = jnp.where((line >= 2) & (odd == h), total[8:], 0.0)
        dot_ref[:, 128 * h : 128 * (h + 1)] = jnp.sum(pick, axis=0, keepdims=True)


def spread():
    a, b = iota((128, 128), 0), iota((128, 128), 1)
    group = lax.bitwise_and(lax.shift_right_logical(a, 1), 15)
    want = 8 * group + 2 * lax.shift_right_logical(a, 5) + lax.bitwise_and(a, 1)
    return jnp.where(b == want, 1.0, 0.0)


def unpack(src, tok, dy):
    perm = spread().astype(BF16)
    for k in range(KT):
        dst, at = (tok, k) if k < KT // 2 else (dy, k - KT // 2)
        block = src[:, k].astype(F32).reshape(GROUPS * 8, 128).astype(BF16)
        dst[: GROUPS * 8, 128 * at : 128 * (at + 1)] = block
    for m in range(KT // 4):
        block = src[:, KT + m].astype(F32).reshape(GROUPS * 8, 128).astype(BF16)
        lines = jnp.dot(perm, block, preferred_element_type=F32).astype(BF16)
        for i in range(4):
            k = 4 * m + i
            dst, at = (tok, k) if k < KT // 2 else (dy, k - KT // 2)
            dst[GROUPS * 8 : GROUPS * CAP, 128 * at : 128 * (at + 1)] = lines[32 * i : 32 * (i + 1)]


def hidden_grads(tok, dy, w):
    rows = tok[:, :D]
    gate_pre = lax.dot_general(rows, w[:HID], CONTRACT_LAST, preferred_element_type=F32)
    up_pre = lax.dot_general(rows, w[HID : 2 * HID], CONTRACT_LAST, preferred_element_type=F32)
    hidden = lax.dot_general(dy[...], w[2 * HID : 3 * HID], CONTRACT_LAST, preferred_element_type=F32)
    square = gate_pre * gate_pre
    th = jnp.tanh(ROOT * (gate_pre + CUBE * square * gate_pre))
    half = 0.5 * (1.0 + th)
    slope = half + 0.5 * gate_pre * (1.0 - th * th) * (ROOT * (1.0 + 3.0 * CUBE * square))
    return (hidden * up_pre * slope).astype(BF16), (hidden * (gate_pre * half)).astype(BF16)


def split_lanes(v):
    high = v.astype(BF16).astype(F32)
    return jnp.where(iota(v.shape, 1) < F, high, v - high).astype(BF16)


def main_kernel(src, mine, other, dot_ref, pt_ref, idx_ref, tok_in, out, cross, gg_ref, ug_ref, lg_ref, dy):
    unpack(src, cross, dy)
    gg, ug = hidden_grads(cross, dy, mine)
    gg_o, ug_o = hidden_grads(cross, dy, other)
    gg_ref[...] = gg
    ug_ref[...] = ug
    cross[:, D : D + HID] = gg_o
    cross[:, D + 256 : D + 256 + HID] = ug_o
    perm = spread().astype(BF16)
    for m in range(KT // 8):
        cols = pl.ds(512 * m, 512)
        part = jnp.dot(gg, mine[:HID, cols], preferred_element_type=F32)
        part = part + jnp.dot(ug, mine[HID : 2 * HID, cols], preferred_element_type=F32)
        part = part + jnp.dot(gg_o, other[:HID, cols], preferred_element_type=F32)
        part = part + jnp.dot(ug_o, other[HID : 2 * HID, cols], preferred_element_type=F32)
        lines = []
        for i in range(4):
            block = part[:, 128 * i : 128 * (i + 1)]
            head = block[: GROUPS * 8].reshape(X, ZL, 8, 128).astype(BF16)
            for z in range(ZL):
                out[:, z * BACK + 4 * m + i] = head[:, z]
            lines.append(block[GROUPS * 8 :])
        tails = jnp.concatenate(lines, axis=0).astype(BF16)
        tails = lax.dot_general(perm, tails, CONTRACT_FIRST, preferred_element_type=F32)
        tails = tails.reshape(X, ZL, 8, 128).astype(BF16)
        for z in range(ZL):
            out[:, z * BACK + KT // 2 + m] = tails[:, z]
    count = jnp.sum(src[:, SENT - 1].astype(F32), axis=0)
    diagonal = iota((E, 128), 0) == iota((E, 128), 1)
    counts = jnp.sum(jnp.where(diagonal, count[:1], 0.0), axis=1, keepdims=True)
    pt = pt_ref[...]
    hot = jnp.where(iota((E, T), 0) == idx_ref[...], 1.0, 0.0)
    grad = hot * dot_ref[...] + AUX * E * counts / (T * E)
    lg = (pt * (grad - jnp.sum(pt * grad, axis=0, keepdims=True))).astype(BF16)
    lg_ref[...] = lg
    twice = jnp.concatenate([tok_in[...], tok_in[...]], axis=0)
    pair = split_lanes(lax.dot_general(lg, twice, CONTRACT_LAST, preferred_element_type=F32))
    for i in range(4):
        for x in range(X):
            out[x, ZL * BACK + i] = pair[8 * i : 8 * (i + 1)]


def merged(got, i):
    pair = jnp.sum(got[:, pl.ds(i, 4)].astype(F32), axis=0).reshape(E, 128)
    return pair + pltpu.roll(pair, F, 1)


def middle_kernel(got, cross, out, bundle, share_ref):
    low = iota((8, 128), 1) < F
    line = iota((8, 128), 0)
    for z in range(ZL):

        def total(k):
            return jnp.sum(got[:, z * BACK + k].astype(F32), axis=0)

        for m in range(KT // 8):
            tail = total(KT // 2 + m)
            for i in range(4):
                k = 4 * m + i
                head = total(k)
                rest = tail if i == 0 else pltpu.roll(tail, 8 - 2 * i, 0)
                rest = jnp.where(line < 2, rest, 0.0)
                out[HOME.index(E * NEAR[z] + 2 * k)] = jnp.where(low, head, pltpu.roll(rest, F, 1)).astype(BF16)
                out[HOME.index(E * NEAR[z] + 2 * k + 1)] = jnp.where(low, pltpu.roll(head, F, 1), rest).astype(BF16)
    share = merged(got, ZL * BACK)
    share_ref[...] = share
    bundle[: GROUPS * CAP, :] = cross[...]
    bundle[GROUPS * CAP :, :] = jnp.zeros((E, WIDE), BF16)
    bundle[GROUPS * CAP :, :128] = split_lanes(share)


def weight_kernel(mine, came, gg, ug, out):
    n = GROUPS * CAP
    for i, m in enumerate((gg, ug)):
        o = came[:n, D + 256 * i : D + 256 * i + HID]
        for c in range(D // 512):
            cols = pl.ds(512 * c, 512)
            grad = lax.dot_general(m[...], mine[:n, cols], CONTRACT_FIRST, preferred_element_type=F32)
            grad = grad + lax.dot_general(o, came[:n, cols], CONTRACT_FIRST, preferred_element_type=F32)
            out[i, :, cols] = grad.astype(BF16)


def folded(a, b):
    pair = a.astype(F32) + b.astype(F32)
    return pair + pltpu.roll(pair, F, 1)


def cores_kernel(share, came, out):
    out[...] = split_lanes(share[...] + folded(came[GROUPS * CAP :, :128], jnp.zeros((E, 128), F32)))


def pairs_kernel(a, b, out):
    out[...] = split_lanes(folded(a[...], b[...]))


def combine_kernel(ret, idx_ref, lg, rw, pair, far, out, router):
    router[...] = folded(pair[...], far[...])[:, :F]
    idx = idx_ref[...]
    _, slot = slots(idx)
    slot = slot.astype(jnp.int32)
    row = iota((E * 8, T), 0)
    mine = lax.shift_right_logical(row, 3) == idx
    c = lax.bitwise_and(row, 7)
    r = jnp.concatenate(
        [sum(ret[HOME.index(E * z + e)].astype(F32) for z in range(ZL)) for e in range(E)], axis=0
    )
    high = r.astype(BF16)
    low = (r - high.astype(F32)).astype(BF16)
    acc = lax.dot_general(rw[...], lg[...], CONTRACT_FIRST, preferred_element_type=F32)
    for h in range(2):
        sel = jnp.where(mine & (c + 8 * h == slot), 1.0, 0.0).astype(BF16)
        for part in (high, low):
            p = lax.dot_general(part, sel, CONTRACT_FIRST, preferred_element_type=F32)
            acc = acc + p[F * h : F * (h + 1)]
    out[...] = acc.astype(BF16)


def local(kernel, outs, ins, flops, scratch=(), hbm=False, kib=8192):
    one = not isinstance(outs, tuple)
    return pl.pallas_call(
        kernel,
        out_shape=outs,
        in_specs=[pl.BlockSpec(memory_space=pltpu.HBM)] * len(ins) if hbm else vmem(len(ins)),
        out_specs=vmem(1)[0] if one else tuple(vmem(len(outs))),
        scratch_shapes=list(scratch),
        cost_estimate=pl.CostEstimate(flops=flops, bytes_accessed=0, transcendentals=0),
        compiler_params=pltpu.CompilerParams(vmem_limit_bytes=kib * 1024),
    )(*ins)


def shape(*dims, dtype=BF16):
    return jax.ShapeDtypeStruct(dims, dtype)


def per_device(tokens, out_grad, expert_out, probs, idx, in_weight, down_weight, router_weight):
    return layer(
        tokens.T,
        out_grad.T,
        expert_out.T,
        probs.T,
        idx.T,
        in_weight,
        down_weight,
        router_weight,
    )


def layer(tok, og, eo, pt, ix, in_weight, down_weight, router_weight):
    swap = [(0, 1), (1, 0)]
    send, tile = local(
        dispatch_kernel,
        (shape(E, 16, 128), shape(8, 128)),
        (tok, og, eo, pt, ix),
        10**7,
        (
            pltpu.VMEM((F, T), BF16),
            pltpu.VMEM((F, T), BF16),
            pltpu.VMEM((F, T), BF16),
            pltpu.VMEM((E, T), F32),
            pltpu.VMEM((1, T), jnp.int32),
            pltpu.SemaphoreType.DMA((5,)),
        ),
        hbm=True,
        kib=DISPATCH_KIB,
    )
    got = lax.all_to_all(send, EX, 0, 0, tiled=True, axis_index_groups=[AWAY])
    mine = local(
        bundle_kernel,
        shape(BUNDLE, D),
        (in_weight[0], down_weight[0], tile),
        10**6,
        (pltpu.VMEM((8, 128), BF16), pltpu.SemaphoreType.DMA((4,))),
        hbm=True,
        kib=60000,
    )
    other = lax.ppermute(mine, "core", swap)
    packed, gate_dot = local(pack_kernel, (shape(SENT, 8, 128), shape(1, T, dtype=F32)), (got, tile, other), 10**7)
    line = lax.all_to_all(jnp.broadcast_to(packed, (ZL, *packed.shape)), "zl", 0, 0, tiled=True, axis_index_groups=[NEAR])
    plane = lax.all_to_all(jnp.broadcast_to(line, (X, *line.shape)), "x", 0, 0, tiled=True, axis_index_groups=[NEAR])
    own = plane.reshape(GROUPS, SENT, 8, 128)
    rows = GROUPS * CAP
    work = 10 * rows * HID * D
    back, cross, gg, ug, lg = local(
        main_kernel,
        (shape(X, TILES, 8, 128), shape(rows, WIDE), shape(rows, HID), shape(rows, HID), shape(E, T)),
        (own, mine, other, gate_dot, pt, ix, tok),
        2 * work,
        (pltpu.VMEM((rows, D), BF16),),
        kib=20000,
    )
    landed = lax.all_to_all(back, "x", 0, 0, tiled=True, axis_index_groups=[NEAR])
    rows_back, bundle, share = local(
        middle_kernel, (shape(ZL * E, 8, 128), shape(CROSS, WIDE), shape(E, 128, dtype=F32)), (landed, cross), 10**6
    )
    ret = lax.all_to_all(rows_back, ("zl", EX), 0, 0, tiled=True, axis_index_groups=[HOME])
    came = lax.ppermute(bundle, "core", swap)
    pair = local(cores_kernel, shape(E, 128), (share, came), 10**5)
    got = lax.ppermute(pair, "zl", [(0, 1), (1, 0), (2, 3), (3, 2)])
    weights = local(weight_kernel, shape(2, HID, D), (bundle, came, gg, ug), work, kib=12000)
    pair = local(pairs_kernel, shape(E, 128), (pair, got), 10**5)
    got = lax.ppermute(pair, "zl", [(0, 2), (2, 0), (1, 3), (3, 1)])
    token_grad, router_sum = local(
        combine_kernel, (shape(F, T), shape(E, F, dtype=F32)), (ret, ix, lg, router_weight.T, pair, got), 10**7
    )
    return token_grad.T, weights[None], router_sum.T


def solution(mesh):
    fine = Mesh(mesh.devices.reshape(ZL, X, CORE, E), (*DP, EX))
    in_specs = (
        P(DP, EX),
        P(DP, EX),
        P(DP, EX),
        P(DP, None),
        P(DP, None),
        P(EX, None, DP, None),
        P(EX, DP, None),
        P(EX, None),
    )
    out_specs = (P(DP, EX), P(EX, None, DP, None), P(EX, None))
    return jax.shard_map(
        per_device, mesh=fine, in_specs=in_specs, out_specs=out_specs, check_vma=False
    )
```

```python
import jax
import jax.numpy as jnp
from jax import lax
from jax.experimental import pallas as pl
from jax.experimental.pallas import tpu as pltpu
from jax.sharding import Mesh, PartitionSpec as P


ZL, X, CORE = 4, 4, 2
EX = "expert"
DP = ("zl", "x", "core")
E = 32
CAP = 10
T = 256
F = 64
D = 2048
KT = 2 * D // 128
AUX = 0.2
ROOT = 0.7978845608028654
CUBE = 0.044715
GROUPS = ZL * X
SENT = KT + KT // 4 + 1
BACK = KT // 2 + KT // 8
TILES = ZL * BACK + 4
HID = 160
BUNDLE = 3 * HID + 16
WIDE = D + 512
AWAY = [4 * y + z for y in (7, 6, 5, 4, 0, 1, 2, 3) for z in (3, 2, 0, 1)]
NEAR = [1, 0, 2, 3]
HOME = [
    E * z + 4 * (4 * far + y) + zh
    for zh in (0, 3, 1, 2)
    for far in (0, 1)
    for z in NEAR
    for y in NEAR
]
DISPATCH_KIB = 60000
CROSS = GROUPS * CAP + E
F32, BF16 = jnp.float32, jnp.bfloat16
CONTRACT_LAST = (((1,), (1,)), ((), ()))
CONTRACT_FIRST = (((0,), (0,)), ((), ()))


def vmem(n):
    return [pl.BlockSpec(memory_space=pltpu.VMEM)] * n


def iota(shape, dim):
    return lax.broadcasted_iota(jnp.int32, shape, dim)


def slots(idx):
    hit = iota((E, T), 0) == idx
    hot = jnp.where(hit, 1.0, 0.0).astype(F32)
    earlier = jnp.where(iota((T, T), 0) < iota((T, T), 1), 1.0, 0.0).astype(BF16)
    before = jnp.dot(hot.astype(BF16), earlier, preferred_element_type=F32)
    return hot, jnp.sum(hot * before, axis=0, keepdims=True)


def dispatch_kernel(tok_h, og_h, eo_h, pt_h, idx_h, out, tile, tok, og, eo, pt, ix, sems):
    copies = [
        pltpu.make_async_copy(a, b, sems.at[i])
        for i, (a, b) in enumerate(
            (
                (idx_h, ix),
                (tok_h, tok),
                (og_h, og),
                (pt_h, pt),
                (eo_h, eo),
            )
        )
    ]
    for c in copies:
        c.start()
    copies[0].wait()
    idx = ix[...]
    hot, slot = slots(idx)
    row = iota((E * 16, T), 0)
    y, z = lax.shift_right_logical(row, 6), lax.bitwise_and(lax.shift_right_logical(row, 4), 3)
    expert = 4 * jnp.where(y < 4, 7 - y, y - 4) + jnp.where(z < 2, 3 - z, z - 2)
    sel = jnp.where(
        (expert == idx)
        & (lax.bitwise_and(row, 15) == slot.astype(jnp.int32)),
        1.0,
        0.0,
    ).astype(BF16)
    wide = jnp.where(iota((128, T), 0) == idx, 1.0, 0.0).astype(BF16)
    counts = lax.dot_general(jnp.ones((8, T), BF16), wide, CONTRACT_LAST, preferred_element_type=F32)
    tile[...] = counts.astype(BF16)
    for c in copies[1:]:
        c.wait()
    gate = jnp.sum(pt[...] * hot, axis=0, keepdims=True)
    grad = og[...].astype(F32)
    gated = (gate * grad).astype(BF16)
    dot = jnp.sum(grad * eo[...].astype(F32), axis=0, keepdims=True)
    both = jnp.concatenate([tok[...], gated], axis=0)
    sent = lax.dot_general(sel, both, CONTRACT_LAST, preferred_element_type=F32)
    h0 = dot.astype(BF16).astype(F32)
    h1 = (dot - h0).astype(BF16).astype(F32)
    h2 = dot - h0 - h1
    line = iota((16, 128), 0)
    extra = jnp.zeros((16, 128), F32)
    for i, h in enumerate((h0, h1, h2)):
        for j in range(2):
            extra = extra + jnp.where(line == CAP + 2 * i + j, h[:, 128 * j : 128 * (j + 1)], 0.0)
    out[...] = (sent.reshape(E, 16, 128) + extra[None]).astype(BF16)


def bundle_kernel(in_h, down_h, tile_h, out, tile, sems):
    copies = [
        pltpu.make_async_copy(a, b, sems.at[i])
        for i, (a, b) in enumerate(
            (
                (tile_h, tile),
                (in_h.at[0], out.at[pl.ds(0, HID)]),
                (in_h.at[1], out.at[pl.ds(HID, HID)]),
                (down_h, out.at[pl.ds(2 * HID, HID)]),
            )
        )
    ]
    for c in copies:
        c.start()
    out[3 * HID :, :] = jnp.zeros((BUNDLE - 3 * HID, D), BF16)
    copies[0].wait()
    out[3 * HID :, :128] = jnp.concatenate([tile[...], tile[...]], axis=0)
    for c in copies[1:]:
        c.wait()


def pack_kernel(got, tile, partner, out, dot_ref):
    low = iota((16, 128), 1) < F
    line = iota((8, 128), 0)
    tail = [jnp.zeros((8, 128), F32) for _ in range(KT // 4)]
    total = jnp.zeros((16, 128), F32)
    for j in range(E // 2):
        a = got[AWAY.index(2 * j)].astype(F32)
        b = got[AWAY.index(2 * j + 1)].astype(F32)
        total = total + a + b
        t = jnp.where(low, a, pltpu.roll(b, F, 1))
        g = jnp.where(low, pltpu.roll(a, F, 1), b)
        for k, v in ((j, t), (j + E // 2, g)):
            out[k] = v[:8].astype(BF16)
            i = k % 4
            rest = v[8:] if i == 0 else pltpu.roll(v[8:], 2 * i, 0)
            tail[k // 4] = jnp.where((line >= 2 * i) & (line < 2 * i + 2), rest, tail[k // 4])
    for m in range(KT // 4):
        out[KT + m] = tail[m].astype(BF16)
    pair = tile[...].astype(F32) + partner[3 * HID : 3 * HID + 8, :128].astype(F32)
    out[KT + KT // 4] = pair.astype(BF16)
    odd = lax.bitwise_and(line, 1)
    for h in range(2):
        pick = jnp.where((line >= 2) & (odd == h), total[8:], 0.0)
        dot_ref[:, 128 * h : 128 * (h + 1)] = jnp.sum(pick, axis=0, keepdims=True)


def spread():
    a, b = iota((128, 128), 0), iota((128, 128), 1)
    group = lax.bitwise_and(lax.shift_right_logical(a, 1), 15)
    want = 8 * group + 2 * lax.shift_right_logical(a, 5) + lax.bitwise_and(a, 1)
    return jnp.where(b == want, 1.0, 0.0)


def unpack(src, tok, dy):
    perm = spread().astype(BF16)
    for k in range(KT):
        dst, at = (tok, k) if k < KT // 2 else (dy, k - KT // 2)
        block = src[:, k].astype(F32).reshape(GROUPS * 8, 128).astype(BF16)
        dst[: GROUPS * 8, 128 * at : 128 * (at + 1)] = block
    for m in range(KT // 4):
        block = src[:, KT + m].astype(F32).reshape(GROUPS * 8, 128).astype(BF16)
        lines = jnp.dot(perm, block, preferred_element_type=F32).astype(BF16)
        for i in range(4):
            k = 4 * m + i
            dst, at = (tok, k) if k < KT // 2 else (dy, k - KT // 2)
            dst[GROUPS * 8 : GROUPS * CAP, 128 * at : 128 * (at + 1)] = lines[32 * i : 32 * (i + 1)]


def hidden_grads(tok, dy, w):
    rows = tok[:, :D]
    gate_pre = lax.dot_general(rows, w[:HID], CONTRACT_LAST, preferred_element_type=F32)
    up_pre = lax.dot_general(rows, w[HID : 2 * HID], CONTRACT_LAST, preferred_element_type=F32)
    hidden = lax.dot_general(dy[...], w[2 * HID : 3 * HID], CONTRACT_LAST, preferred_element_type=F32)
    square = gate_pre * gate_pre
    th = jnp.tanh(ROOT * (gate_pre + CUBE * square * gate_pre))
    half = 0.5 * (1.0 + th)
    slope = half + 0.5 * gate_pre * (1.0 - th * th) * (ROOT * (1.0 + 3.0 * CUBE * square))
    return (hidden * up_pre * slope).astype(BF16), (hidden * (gate_pre * half)).astype(BF16)


def split_lanes(v):
    high = v.astype(BF16).astype(F32)
    return jnp.where(iota(v.shape, 1) < F, high, v - high).astype(BF16)


def main_kernel(src, mine, other, dot_ref, pt_ref, idx_ref, tok_in, out, cross, gg_ref, ug_ref, lg_ref, dy):
    unpack(src, cross, dy)
    gg, ug = hidden_grads(cross, dy, mine)
    gg_o, ug_o = hidden_grads(cross, dy, other)
    gg_ref[...] = gg
    ug_ref[...] = ug
    cross[:, D : D + HID] = gg_o
    cross[:, D + 256 : D + 256 + HID] = ug_o
    perm = spread().astype(BF16)
    for m in range(KT // 8):
        cols = pl.ds(512 * m, 512)
        part = jnp.dot(gg, mine[:HID, cols], preferred_element_type=F32)
        part = part + jnp.dot(ug, mine[HID : 2 * HID, cols], preferred_element_type=F32)
        part = part + jnp.dot(gg_o, other[:HID, cols], preferred_element_type=F32)
        part = part + jnp.dot(ug_o, other[HID : 2 * HID, cols], preferred_element_type=F32)
        lines = []
        for i in range(4):
            block = part[:, 128 * i : 128 * (i + 1)]
            head = block[: GROUPS * 8].reshape(X, ZL, 8, 128).astype(BF16)
            for z in range(ZL):
                out[:, z * BACK + 4 * m + i] = head[:, z]
            lines.append(block[GROUPS * 8 :])
        tails = jnp.concatenate(lines, axis=0).astype(BF16)
        tails = lax.dot_general(perm, tails, CONTRACT_FIRST, preferred_element_type=F32)
        tails = tails.reshape(X, ZL, 8, 128).astype(BF16)
        for z in range(ZL):
            out[:, z * BACK + KT // 2 + m] = tails[:, z]
    count = jnp.sum(src[:, SENT - 1].astype(F32), axis=0)
    diagonal = iota((E, 128), 0) == iota((E, 128), 1)
    counts = jnp.sum(jnp.where(diagonal, count[:1], 0.0), axis=1, keepdims=True)
    pt = pt_ref[...]
    hot = jnp.where(iota((E, T), 0) == idx_ref[...], 1.0, 0.0)
    grad = hot * dot_ref[...] + AUX * E * counts / (T * E)
    lg = (pt * (grad - jnp.sum(pt * grad, axis=0, keepdims=True))).astype(BF16)
    lg_ref[...] = lg
    twice = jnp.concatenate([tok_in[...], tok_in[...]], axis=0)
    pair = split_lanes(lax.dot_general(lg, twice, CONTRACT_LAST, preferred_element_type=F32))
    for i in range(4):
        for x in range(X):
            out[x, ZL * BACK + i] = pair[8 * i : 8 * (i + 1)]


def merged(got, i):
    pair = jnp.sum(got[:, pl.ds(i, 4)].astype(F32), axis=0).reshape(E, 128)
    return pair + pltpu.roll(pair, F, 1)


def middle_kernel(got, cross, out, bundle, share_ref):
    low = iota((8, 128), 1) < F
    line = iota((8, 128), 0)
    for z in range(ZL):

        def total(k):
            return jnp.sum(got[:, z * BACK + k].astype(F32), axis=0)

        for m in range(KT // 8):
            tail = total(KT // 2 + m)
            for i in range(4):
                k = 4 * m + i
                head = total(k)
                rest = tail if i == 0 else pltpu.roll(tail, 8 - 2 * i, 0)
                rest = jnp.where(line < 2, rest, 0.0)
                out[HOME.index(E * NEAR[z] + 2 * k)] = jnp.where(low, head, pltpu.roll(rest, F, 1)).astype(BF16)
                out[HOME.index(E * NEAR[z] + 2 * k + 1)] = jnp.where(low, pltpu.roll(head, F, 1), rest).astype(BF16)
    share = merged(got, ZL * BACK)
    share_ref[...] = share
    bundle[: GROUPS * CAP, :] = cross[...]
    bundle[GROUPS * CAP :, :] = jnp.zeros((E, WIDE), BF16)
    bundle[GROUPS * CAP :, :128] = split_lanes(share)


def weight_kernel(mine, came, gg, ug, out):
    n = GROUPS * CAP
    for i, m in enumerate((gg, ug)):
        o = came[:n, D + 256 * i : D + 256 * i + HID]
        for c in range(D // 512):
            cols = pl.ds(512 * c, 512)
            grad = lax.dot_general(m[...], mine[:n, cols], CONTRACT_FIRST, preferred_element_type=F32)
            grad = grad + lax.dot_general(o, came[:n, cols], CONTRACT_FIRST, preferred_element_type=F32)
            out[i, :, cols] = grad.astype(BF16)


def folded(a, b):
    pair = a.astype(F32) + b.astype(F32)
    return pair + pltpu.roll(pair, F, 1)


def cores_kernel(share, came, out):
    out[...] = split_lanes(share[...] + folded(came[GROUPS * CAP :, :128], jnp.zeros((E, 128), F32)))


def pairs_kernel(a, b, out):
    out[...] = split_lanes(folded(a[...], b[...]))


def combine_kernel(ret, idx_ref, lg, rw, pair, far, out, router):
    router[...] = folded(pair[...], far[...])[:, :F]
    idx = idx_ref[...]
    _, slot = slots(idx)
    slot = slot.astype(jnp.int32)
    row = iota((E * 8, T), 0)
    mine = lax.shift_right_logical(row, 3) == idx
    c = lax.bitwise_and(row, 7)
    r = jnp.concatenate(
        [sum(ret[HOME.index(E * z + e)].astype(F32) for z in range(ZL)) for e in range(E)], axis=0
    )
    high = r.astype(BF16)
    low = (r - high.astype(F32)).astype(BF16)
    acc = lax.dot_general(rw[...], lg[...], CONTRACT_FIRST, preferred_element_type=F32)
    for h in range(2):
        sel = jnp.where(mine & (c + 8 * h == slot), 1.0, 0.0).astype(BF16)
        for part in (high, low):
            p = lax.dot_general(part, sel, CONTRACT_FIRST, preferred_element_type=F32)
            acc = acc + p[F * h : F * (h + 1)]
    out[...] = acc.astype(BF16)


def local(kernel, outs, ins, flops, scratch=(), hbm=False, kib=8192):
    one = not isinstance(outs, tuple)
    return pl.pallas_call(
        kernel,
        out_shape=outs,
        in_specs=[pl.BlockSpec(memory_space=pltpu.HBM)] * len(ins) if hbm else vmem(len(ins)),
        out_specs=vmem(1)[0] if one else tuple(vmem(len(outs))),
        scratch_shapes=list(scratch),
        cost_estimate=pl.CostEstimate(flops=flops, bytes_accessed=0, transcendentals=0),
        compiler_params=pltpu.CompilerParams(vmem_limit_bytes=kib * 1024),
    )(*ins)


def shape(*dims, dtype=BF16):
    return jax.ShapeDtypeStruct(dims, dtype)


def per_device(tokens, out_grad, expert_out, probs, idx, in_weight, down_weight, router_weight):
    return layer(
        tokens.T,
        out_grad.T,
        expert_out.T,
        probs.T,
        idx.T,
        in_weight,
        down_weight,
        router_weight,
    )


def layer(tok, og, eo, pt, ix, in_weight, down_weight, router_weight):
    swap = [(0, 1), (1, 0)]
    send, tile = local(
        dispatch_kernel,
        (shape(E, 16, 128), shape(8, 128)),
        (tok, og, eo, pt, ix),
        10**7,
        (
            pltpu.VMEM((F, T), BF16),
            pltpu.VMEM((F, T), BF16),
            pltpu.VMEM((F, T), BF16),
            pltpu.VMEM((E, T), F32),
            pltpu.VMEM((1, T), jnp.int32),
            pltpu.SemaphoreType.DMA((5,)),
        ),
        hbm=True,
        kib=DISPATCH_KIB,
    )
    got = lax.all_to_all(send, EX, 0, 0, tiled=True, axis_index_groups=[AWAY])
    mine = local(
        bundle_kernel,
        shape(BUNDLE, D),
        (in_weight[0], down_weight[0], tile),
        10**6,
        (pltpu.VMEM((8, 128), BF16), pltpu.SemaphoreType.DMA((4,))),
        hbm=True,
        kib=60000,
    )
    other = lax.ppermute(mine, "core", swap)
    packed, gate_dot = local(pack_kernel, (shape(SENT, 8, 128), shape(1, T, dtype=F32)), (got, tile, other), 10**7)
    line = lax.all_to_all(jnp.broadcast_to(packed, (ZL, *packed.shape)), "zl", 0, 0, tiled=True, axis_index_groups=[NEAR])
    plane = lax.all_to_all(jnp.broadcast_to(line, (X, *line.shape)), "x", 0, 0, tiled=True, axis_index_groups=[NEAR])
    own = plane.reshape(GROUPS, SENT, 8, 128)
    rows = GROUPS * CAP
    work = 10 * rows * HID * D
    back, cross, gg, ug, lg = local(
        main_kernel,
        (shape(X, TILES, 8, 128), shape(rows, WIDE), shape(rows, HID), shape(rows, HID), shape(E, T)),
        (own, mine, other, gate_dot, pt, ix, tok),
        2 * work,
        (pltpu.VMEM((rows, D), BF16),),
        kib=20000,
    )
    landed = lax.all_to_all(back, "x", 0, 0, tiled=True, axis_index_groups=[NEAR])
    rows_back, bundle, share = local(
        middle_kernel, (shape(ZL * E, 8, 128), shape(CROSS, WIDE), shape(E, 128, dtype=F32)), (landed, cross), 10**6
    )
    ret = lax.all_to_all(rows_back, ("zl", EX), 0, 0, tiled=True, axis_index_groups=[HOME])
    came = lax.ppermute(bundle, "core", swap)
    pair = local(cores_kernel, shape(E, 128), (share, came), 10**5)
    got = lax.ppermute(pair, "zl", [(0, 1), (1, 0), (2, 3), (3, 2)])
    weights = local(weight_kernel, shape(2, HID, D), (bundle, came, gg, ug), work, kib=12000)
    pair = local(pairs_kernel, shape(E, 128), (pair, got), 10**5)
    got = lax.ppermute(pair, "zl", [(0, 2), (2, 0), (1, 3), (3, 1)])
    token_grad, router_sum = local(
        combine_kernel, (shape(F, T), shape(E, F, dtype=F32)), (ret, ix, lg, router_weight.T, pair, got), 10**7
    )
    return token_grad.T, weights[None], router_sum.T


def solution(mesh):
    fine = Mesh(mesh.devices.reshape(ZL, X, CORE, E), (*DP, EX))
    in_specs = (
        P(DP, EX),
        P(DP, EX),
        P(DP, EX),
        P(DP, None),
        P(DP, None),
        P(EX, None, DP, None),
        P(EX, DP, None),
        P(EX, None),
    )
    out_specs = (P(DP, EX), P(EX, None, DP, None), P(EX, None))
    return jax.shard_map(
        per_device, mesh=fine, in_specs=in_specs, out_specs=out_specs, check_vma=False
    )
```
